32 devices in a mesh: parts: 2 (over y), patch: 4 (over z), sub: 4 (over x, core).
Axes of the slice: x: 2, y: 2, z: 4, core: 2. Of those that a mesh axis runs over, the one named last changes fastest.
Arguments:
- node_latents: bfloat16 [4096, 512], P(('parts', 'patch', 'sub')), parts along dimension 0, may hold values from -6 to 6
- edge_latents: bfloat16 [16384, 512], P(('parts', 'patch', 'sub')), parts along dimension 0, may hold values from -6 to 6
- coarse_edges: bfloat16 [2048, 512], P(('parts', 'patch', 'sub')), parts along dimension 0, may hold values from -6 to 6
- w_edge_in: bfloat16 [1536, 512], replicated, may hold values from -0.15625 to 0.15625
- w_edge_out: bfloat16 [512, 512], replicated, may hold values from -0.25 to 0.25
- w_node_in: bfloat16 [1024, 512], replicated, may hold values from -0.1875 to 0.1875
- w_node_out: bfloat16 [512, 512], replicated, may hold values from -0.25 to 0.25
- fine_senders: int32 [16384], P(('parts', 'patch', 'sub')), parts along dimension 0, may hold values from 0 to 159
- fine_receivers: int32 [16384], P(('parts', 'patch', 'sub')), parts along dimension 0, may hold values from -1 to 127, as said below
- halo_lists: int32 [32, 2, 16], P(('parts', 'patch', 'sub')), parts along dimension 0, may hold values from 0 to 127, as said below
- coarse_senders: int32 [2048], P(('parts', 'patch', 'sub')), parts along dimension 0, may hold values from 0 to 63
- coarse_receivers: int32 [2048], P(('parts', 'patch', 'sub')), parts along dimension 0, may hold values from 0 to 63
Outputs:
- new_nodes: bfloat16 [4096, 512], P(('parts', 'patch', 'sub')), parts along dimension 0
- new_edges: bfloat16 [16384, 512], P(('parts', 'patch', 'sub')), parts along dimension 0
- new_coarse: bfloat16 [2048, 512], P(('parts', 'patch', 'sub')), parts along dimension 0
The draws below stay inside these ranges and needn't reach their ends.
There are 2 independent parts, one for each index of `parts`. The reference program is written for one: setup_inputs(seed, part) draws one part's arguments, and reference() takes and returns one part's arrays. A program takes and returns all parts, laid end to end along the dimension named above; an argument that names none is the same for every part. Nothing has to cross between parts.
Inputs may be any that keep to these rules, and one draw needn't show every extreme that they name: `fine_receivers`: in each device's block of 512 slots the used slots come first and name a local row; the rest hold -1. At least half of a device's slots are used, and some device uses all of them. `halo_lists`: each of a device's two lists holds 16 distinct local rows.
All inputs are finite; a program needn't handle non-finite values.
Results may differ from the reference program's by a relative error of at most 0.0053.
Values may be sent and summed in bfloat16 or wider, within the bound.
A program may use at most 64 MiB of HBM per device.

```python
import jax
import jax.numpy as jnp
from jax import lax

D = 512
NODE_DEV = 128
HALO = 16
CO_DEV = 4
GROUP = 16
EDGE_DEV = 512
CEDGE_DEV = 64
NODES = 2048
EDGES = 8192
CEDGES = 1024
N_PATCH = 4
N_SUB = 4


def draw_fine_receivers(key, part):
    key_counts = jax.random.fold_in(key, 11)
    key_full = jax.random.fold_in(key, 12)
    key_rows = jax.random.fold_in(key, 13)
    counts = jax.random.randint(key_counts, (GROUP,), EDGE_DEV // 2, EDGE_DEV + 1)
    full = jax.random.randint(key_full, (), 0, GROUP)
    counts = jnp.where(jnp.arange(GROUP) == full, EDGE_DEV, counts)
    rows = jax.random.randint(key_rows, (GROUP, EDGE_DEV), 0, NODE_DEV)
    slots = jnp.arange(EDGE_DEV)[None, :]
    return jnp.where(slots < counts[:, None], rows, -1).reshape(GROUP * EDGE_DEV).astype(jnp.int32)


def draw_halo_lists(key, part):
    keys = jax.random.split(jax.random.fold_in(key, 21), GROUP * 2)
    chosen = jax.vmap(lambda single: jax.random.permutation(single, NODE_DEV)[:HALO])(keys)
    return chosen.reshape(GROUP, 2, HALO).astype(jnp.int32)


def whole_part_ids(key):
    return jax.random.randint(key, (GROUP * CEDGE_DEV,), 0, GROUP * CO_DEV).astype(jnp.int32)


def draw_coarse_senders(key, part):
    return whole_part_ids(jax.random.fold_in(key, 31))


def draw_coarse_receivers(key, part):
    return whole_part_ids(jax.random.fold_in(key, 32))


def plant(result, stream_key, least, high):
    index_at = [jax.random.randint(jax.random.fold_in(stream_key, axis), (), 0, length) for axis, length in enumerate(result.shape)]
    longest = result.shape.index(max(result.shape))
    neighbour = index_at[:longest] + [(index_at[longest] + 1) % result.shape[longest]] + index_at[longest + 1:]
    return result.at[tuple(index_at)].set(least).at[tuple(neighbour)].set(high)


def steps_of(own_key, dims, cuts, least, high):
    def one(position, shards_of):
        steps = jax.random.uniform(jax.random.fold_in(jax.random.fold_in(own_key, 6), position), (shards_of,), jnp.float32, least / len(cuts), high / len(cuts))
        return jnp.repeat(jnp.exp(steps), dims[position] // shards_of).reshape((-1,) + (1,) * (len(dims) - position - 1))

    factor_of = one(*cuts[0])
    for cut in cuts[1:]:
        factor_of = factor_of * one(*cut)
    return factor_of


def gaussian(stream_key, dims, spread, most, pieces=(), kind=jnp.bfloat16):
    array = spread * jax.random.normal(stream_key, dims, jnp.float32)
    if pieces:
        array = array * steps_of(stream_key, dims, pieces, -0.22, 0.18)
    return jnp.clip(array, -most, most).astype(kind)


def setup_inputs(seed: int = 0, part: int = 0) -> dict:
    key_list = jax.random.split(jax.random.key(seed), 13)
    part_splits = jax.random.split(jax.random.fold_in(key_list[12], part), 13)
    node_latents = gaussian(part_splits[0], (NODES, D), 1.0, 6.0, ((0, 16),))
    edge_latents = gaussian(part_splits[1], (EDGES, D), 1.0, 6.0, ((0, 16),))
    coarse_edges = gaussian(part_splits[2], (CEDGES, D), 1.0, 6.0, ((0, 16),))
    w_edge_in = gaussian(key_list[3], (3 * D, D), (3 * D) ** -0.5, 0.15625)
    w_edge_out = gaussian(key_list[4], (D, D), D ** -0.5, 0.25)
    w_node_in = gaussian(key_list[5], (2 * D, D), (2 * D) ** -0.5, 0.1875)
    w_node_out = gaussian(key_list[6], (D, D), D ** -0.5, 0.25)
    fine_senders = plant(jax.random.randint(part_splits[7], (EDGES,), 0, NODE_DEV + 2 * HALO), jax.random.fold_in(part_splits[7], 1), 0, (NODE_DEV + 2 * HALO) - 1).astype(jnp.int32)
    fine_receivers = draw_fine_receivers(jax.random.fold_in(jax.random.fold_in(key_list[12], part), 71), part)
    halo_lists = draw_halo_lists(jax.random.fold_in(jax.random.fold_in(key_list[12], part), 71), part)
    coarse_senders = draw_coarse_senders(jax.random.fold_in(jax.random.fold_in(key_list[12], part), 71), part)
    coarse_receivers = draw_coarse_receivers(jax.random.fold_in(jax.random.fold_in(key_list[12], part), 71), part)
    return dict(node_latents=node_latents, edge_latents=edge_latents, coarse_edges=coarse_edges, w_edge_in=w_edge_in, w_edge_out=w_edge_out, w_node_in=w_node_in, w_node_out=w_node_out, fine_senders=fine_senders, fine_receivers=fine_receivers, halo_lists=halo_lists, coarse_senders=coarse_senders, coarse_receivers=coarse_receivers)


def norm_rows(values):
    mean = lax.optimization_barrier(jnp.mean(values, axis=-1, keepdims=True))
    centred = values - mean
    return centred * lax.rsqrt(lax.optimization_barrier(jnp.mean(centred * centred, axis=-1, keepdims=True)) + 1e-05)

def edge_delta(inputs, w_edge_in, w_edge_out):
    pre = jnp.dot(inputs, w_edge_in, preferred_element_type=jnp.float32)
    hidden = jax.nn.silu(pre).astype(jnp.bfloat16)
    return norm_rows(jnp.dot(hidden, w_edge_out, preferred_element_type=jnp.float32))

def reference(node_latents, edge_latents, coarse_edges, w_edge_in, w_edge_out, w_node_in, w_node_out, fine_senders, fine_receivers, halo_lists, coarse_senders, coarse_receivers):
    group = N_PATCH * N_SUB
    nodes = node_latents.reshape(group, NODE_DEV, D)
    sent_next = jax.vmap(lambda block, lists: block[lists[0]])(nodes, halo_lists)
    sent_prev = jax.vmap(lambda block, lists: block[lists[1]])(nodes, halo_lists)
    extended = jnp.concatenate([jnp.roll(sent_next, 1, axis=0), nodes, jnp.roll(sent_prev, -1, axis=0)], axis=1)
    coarse_latents = nodes[:, :CO_DEV].reshape(group * CO_DEV, D)

    def per_device(items):
        ext, own, edges, cedges, senders, receivers, csend, crecv = items
        fine_in = jnp.concatenate([edges, ext[senders], own[jnp.maximum(receivers, 0)]], axis=1)
        coarse_in = jnp.concatenate([cedges, coarse_latents[csend], coarse_latents[crecv]], axis=1)
        delta = edge_delta(jnp.concatenate([fine_in, coarse_in], axis=0), w_edge_in, w_edge_out)
        valid = (receivers >= 0)[:, None]
        fine_new = (edges.astype(jnp.float32) + jnp.where(valid, delta[:EDGE_DEV], 0.0)).astype(jnp.bfloat16)
        coarse_new = (cedges.astype(jnp.float32) + delta[EDGE_DEV:]).astype(jnp.bfloat16)
        onehot = (jnp.arange(NODE_DEV, dtype=jnp.int32)[:, None] == receivers[None, :]).astype(jnp.bfloat16)
        fine_agg = jnp.dot(onehot, fine_new, preferred_element_type=jnp.float32)
        return (fine_new, coarse_new, fine_agg)
    fine_new, coarse_new, fine_agg = lax.map(per_device, (extended, nodes, edge_latents.reshape(group, EDGE_DEV, D), coarse_edges.reshape(group, CEDGE_DEV, D), fine_senders.reshape(group, EDGE_DEV), fine_receivers.reshape(group, EDGE_DEV), coarse_senders.reshape(group, CEDGE_DEV), coarse_receivers.reshape(group, CEDGE_DEV)))
    coarse_flat = coarse_new.reshape(group * CEDGE_DEV, D)
    coarse_agg = jax.ops.segment_sum(coarse_flat.astype(jnp.float32), coarse_receivers, group * CO_DEV)
    aggregate = fine_agg.at[:, :CO_DEV].add(coarse_agg.reshape(group, CO_DEV, D))
    aggregate = aggregate.reshape(group * NODE_DEV, D).astype(jnp.bfloat16)
    pre = jnp.dot(jnp.concatenate([node_latents, aggregate], axis=1), w_node_in, preferred_element_type=jnp.float32)
    hidden = jax.nn.silu(pre).astype(jnp.bfloat16)
    delta = norm_rows(jnp.dot(hidden, w_node_out, preferred_element_type=jnp.float32))
    new_nodes = (node_latents.astype(jnp.float32) + delta).astype(jnp.bfloat16)
    return (new_nodes, fine_new.reshape(group * EDGE_DEV, D), coarse_flat)
```

```python
import functools

import jax
import jax.numpy as jnp
from jax import lax
from jax.experimental import pallas as pl
from jax.experimental.pallas import tpu as pltpu
from jax.sharding import PartitionSpec as P

CO_DEV = 4
FIRST = 16
F32 = jnp.float32
BF16 = jnp.bfloat16
MESH = pl.DeviceIdType.MESH


def dot(a, b, dims=((1,), (0,))):
    return lax.dot_general(a, b, (dims, ((), ())), preferred_element_type=F32)


def silu(v):
    half = 0.5 * v
    return (half + half * jnp.tanh(half)).astype(BF16)


def norm_rows(values):
    mean = jnp.mean(values, axis=-1, keepdims=True)
    centred = values - mean
    return centred * lax.rsqrt(jnp.mean(centred * centred, axis=-1, keepdims=True) + 1e-05)


def column(row):
    n = row.shape[1]
    wide = jnp.broadcast_to(row.astype(F32), (8, n))
    return jnp.transpose(wide)[:, :1]


def hot(col, first, count):
    lanes = lax.broadcasted_iota(jnp.int32, (col.shape[0], count), 1) + first
    return (col == lanes.astype(F32)).astype(BF16)


def hot_t(row, count):
    rows = lax.broadcasted_iota(jnp.int32, (count, row.shape[1]), 0)
    return (rows == row).astype(BF16)


def each(count, step):
    if count <= 16:
        for i in range(count):
            step(i)
    else:
        def run(i, carry):
            step(i)
            return carry

        lax.fori_loop(0, count, run, 0)


def node_rows(rows, pre, w_out):
    return (rows.astype(F32) + norm_rows(dot(silu(pre), w_out))).astype(BF16)


def kernel(
    n_patch, n_sub,
    nodes_h, edges_h, ced_h, wei_h, weo_h, wni_h, wno_h, fs_h, fr_h, hl_h, cs_h, cr_h,
    n_rows, ne_v, nc_v, nodes_v, n_pre, top, wni_v, wno_v,
    edges_v, ced_v, wei_v, weo_v, fs_v, fr_v, hl_v, cs_v, cr_v,
    mate_v, mate_new, mate_cs, mate_cr,
    heads_r, heads_f, halo_s, halo_r, part_f, part_s, part_r,
    acc, in_sem, ag_s, ag_r, halo_ss, halo_rs, rs_s, rs_r, mate_s, mate_r, back_s, back_r, near, go,
):
    half_p = n_patch // 2
    group, half = n_patch * n_sub, half_p * n_sub
    mp, ms = lax.axis_index("patch"), lax.axis_index("sub")
    me = mp * n_sub + ms
    hub = mp < half_p
    leaf = mp >= half_p
    nodes_n, d = nodes_v.shape
    edges_n = edges_v.shape[0]
    halo = halo_s.shape[1]
    co = heads_r.shape[1]
    count = ced_v.shape[0]

    def rows_of(i):
        start = i * 2 * co
        return pl.ds(start if isinstance(i, int) else pl.multiple_of(start, 2 * co), 2 * co)

    def turn(i, by, n):
        at = i + by
        return jnp.where(at >= n, at - n, at)

    def device(p, s):
        return {"device_id": {"patch": p, "sub": s}, "device_id_type": MESH}

    def device_of(i):
        return device(lax.div(i, n_sub), lax.rem(i, n_sub))

    def patch(p, step, own=True):
        for j in range(1, n_sub):
            step(p, turn(ms, j, n_sub))
        if own:
            step(p, ms)

    def other_hubs(step):
        each(half_p - 1, lambda i: patch(turn(mp, i + 1, half_p), step))
        patch(mp, step, own=False)

    def leaves(step):
        each(half_p, lambda i: patch(n_patch - 1 - i, step))

    barrier = pltpu.get_barrier_semaphore()

    @pl.when(hub)
    def _():
        def hail(p, s):
            pl.semaphore_signal(barrier, inc=1, **device(p, s))

        other_hubs(hail)
        leaves(hail)

    row = nodes_h.at[pl.ds(0, co)]

    def send_head(p, s):
        pltpu.make_async_remote_copy(
            src_ref=row, dst_ref=heads_r.at[me], send_sem=ag_s, recv_sem=ag_r,
            **device(p, s)).start()

    to_hub = device(mp - half_p, ms)
    visit = [
        pltpu.make_async_remote_copy(
            src_ref=src, dst_ref=dst, send_sem=mate_s.at[i], recv_sem=mate_r.at[i], **to_hub)
        for i, (src, dst) in enumerate(((cs_h, mate_cs), (cr_h, mate_cr), (ced_h, mate_v)))
    ]
    back = pltpu.make_async_remote_copy(
        src_ref=mate_new, dst_ref=mate_v, send_sem=back_s, recv_sem=back_r,
        **device(mp + half_p, ms))

    @pl.when(leaf)
    def _():
        pl.semaphore_wait(barrier, half)
        for copy in visit:
            copy.start()
        each(half_p, lambda p: patch(p, send_head))
        pl.semaphore_signal(near, inc=1, **to_hub)
        for by in (1, group - 1):
            beside = turn(me, by, group)
            pl.semaphore_signal(
                near, inc=1, **device_of(jnp.where(beside < half, beside, beside - half)))

    pairs = [
        (nodes_h, nodes_v), (hl_h, hl_v), (fs_h, fs_v), (fr_h, fr_v), (cs_h, cs_v), (cr_h, cr_v),
        (wei_h, wei_v), (edges_h, edges_v), (ced_h, ced_v),
        (weo_h, weo_v), (wni_h, wni_v), (wno_h, wno_v),
    ]
    loads = [pltpu.make_async_copy(h, v, in_sem.at[i]) for i, (h, v) in enumerate(pairs)]
    for copy in loads:
        copy.start()
    (l_nodes, l_hl, l_fs, l_fr, l_cs, l_cr, l_wei, l_edges, l_ced, l_weo, l_wni, l_wno) = loads

    l_nodes.wait()
    nodes = nodes_v[...]
    l_hl.wait()
    for side in range(2):
        pick = hot_t(hl_v[0, side:side + 1, :], nodes_n)
        halo_s[side] = dot(pick, nodes, ((0,), (0,))).astype(BF16)

    @pl.when(hub)
    def _():
        heads_r[me] = nodes_v[:co]
        pl.semaphore_wait(barrier, half - 1)
        other_hubs(send_head)

    halos, soon = [], []
    for side, by in ((0, 1), (1, group - 1)):
        to = turn(me, by, group)
        soon.append(to < half)
        halos.append(pltpu.make_async_remote_copy(
            src_ref=halo_s.at[side], dst_ref=halo_r.at[side],
            send_sem=halo_ss.at[side], recv_sem=halo_rs.at[side], **device_of(to)))
        pl.when(soon[-1])(halos[-1].start)

    l_fs.wait()
    l_fr.wait()
    l_cs.wait()
    l_cr.wait()
    fs, fr = fs_v[...], fr_v[...]
    fs_col = column(jnp.where(fs < halo, fs + (nodes_n + halo), fs - halo))
    fr_col = column(fr)

    l_wei.wait()
    own = jnp.concatenate(
        [dot(nodes, wei_v[d:2 * d]).astype(BF16), dot(nodes, wei_v[2 * d:]).astype(BF16)], axis=0)
    sel = jnp.concatenate([hot(fs_col, 0, nodes_n), hot(fr_col, 0, nodes_n)], axis=1)
    l_edges.wait()
    l_ced.wait()
    acc[...] = dot(edges_v[...], wei_v[:d]) + dot(sel, own)
    l_weo.wait()
    l_wni.wait()
    l_wno.wait()

    @pl.when(hub)
    def _():
        pl.semaphore_wait(near, 3)
        pl.semaphore_signal(go, inc=1, **device(mp + half_p, ms))

    @pl.when(leaf)
    def _():
        pl.semaphore_wait(go, 1)

    for early, copy in zip(soon, halos):
        pl.when(jnp.logical_not(early))(copy.start)

    @pl.when(hub)
    def _():
        ced = ced_v[...]
        ced_pre = dot(ced, wei_v[:d])
        visit[0].wait_recv()
        visit[1].wait_recv()
        cs = jnp.concatenate([cs_v[...], mate_cs[...]], axis=1)
        cr = jnp.concatenate([cr_v[...], mate_cr[...]], axis=1)
        picks = hot_t(cr, group * co)
        ends = jnp.concatenate(
            [hot(column(cs), 0, group * co), hot(column(cr), 0, group * co)], axis=0)

        many = heads_r.at[pl.ds(0, group - 1)]
        pltpu.make_async_copy(many, many, ag_r).wait()

        def flat(i):
            both = jnp.concatenate(
                [heads_r[2 * i].astype(F32), heads_r[2 * i + 1].astype(F32)], axis=0)
            heads_f[rows_of(i), :] = both

        each(group // 2, flat)
        heads = heads_f[...].astype(BF16)
        c_ends = dot(ends, heads).astype(BF16)
        c_in = jnp.concatenate([c_ends[:2 * count], c_ends[2 * count:]], axis=1)
        c_pre = dot(c_in, wei_v[d:])
        visit[2].wait_recv()
        mate = mate_v[...]
        both = jnp.concatenate([ced, mate], axis=0)
        c_hid = silu(c_pre + jnp.concatenate([ced_pre, dot(mate, wei_v[:d])], axis=0))
        c_new = (both.astype(F32) + norm_rows(dot(c_hid, weo_v[...]))).astype(BF16)
        part_f[...] = dot(picks, c_new)

        def pack(i):
            both = part_f[rows_of(i), :].astype(BF16)
            part_s[2 * i] = both[:co]
            part_s[2 * i + 1] = both[co:]

        each(group // 2, pack)

        def send_part(p, s):
            pltpu.make_async_remote_copy(
                src_ref=part_s.at[p * n_sub + s], dst_ref=part_r.at[me],
                send_sem=rs_s, recv_sem=rs_r, **device(p, s)).start()

        other_hubs(send_part)
        leaves(send_part)
        mate_new[...] = c_new[count:]
        back.start()
        part_r[me] = part_s[me]
        nc_v[...] = c_new[:count]

    for copy in halos:
        copy.wait_recv()
    far = dot(jnp.concatenate([halo_r[1], halo_r[0]], axis=0), wei_v[d:2 * d]).astype(BF16)
    hid = silu(acc[...] + dot(hot(fs_col, nodes_n, 2 * halo), far))
    delta = norm_rows(dot(hid, weo_v[...]))
    e_new = (edges_v[...].astype(F32) + jnp.where(fr_col >= 0.0, delta, 0.0)).astype(BF16)
    ne_v[...] = e_new
    fine = dot(hot_t(fr, nodes_n), e_new)

    pre = dot(nodes, wni_v[:d])
    n_rows[...] = node_rows(nodes, pre + dot(fine.astype(BF16), wni_v[d:]), wno_v[...])
    first = top.shape[0]
    n_pre[...] = pre[:first]
    top[...] = fine[:first]

    for copy in halos:
        copy.wait_send()

    def await_rows(number, sem):
        span = heads_r.at[pl.ds(0, number)]
        pltpu.make_async_copy(span, span, sem).wait()

    @pl.when(hub)
    def _():
        await_rows(half - 1, ag_s)
        await_rows(group - 1, rs_s)
        back.wait_send()
        await_rows(half - 1, rs_r)

    @pl.when(leaf)
    def _():
        await_rows(half, ag_s)
        for copy in visit:
            copy.wait_send()
        back.wait_recv()
        nc_v[...] = mate_v[...]
        await_rows(half, rs_r)

    top[:co] += jnp.sum(part_r[...].astype(F32), axis=0)


def finish(n_rows, ne_v, nc_v, nodes_v, n_pre, top, wni_v, wno_v, nn_h, ne_h, nc_h, first_v, sem):
    first, d = top.shape
    n = n_rows.shape[0]
    copies = [
        pltpu.make_async_copy(ne_v, ne_h, sem.at[0]),
        pltpu.make_async_copy(nc_v, nc_h, sem.at[1]),
        pltpu.make_async_copy(n_rows.at[pl.ds(first, n - first)], nn_h.at[pl.ds(first, n - first)],
                              sem.at[2]),
    ]
    for copy in copies:
        copy.start()
    pre = n_pre[...] + dot(top[...].astype(BF16), wni_v[d:])
    first_v[...] = node_rows(nodes_v[:first], pre, wno_v[...])
    copies.append(pltpu.make_async_copy(first_v, nn_h.at[pl.ds(0, first)], sem.at[3]))
    copies[-1].start()
    for copy in copies:
        copy.wait()


def body(n_patch, n_sub, *args):
    nodes, edges, ced, wei, weo, wni, wno, fs, fr, hl, cs, cr = args
    fs, fr, cs, cr = (x.reshape(1, -1) for x in (fs, fr, cs, cr))
    operands = (nodes, edges, ced, wei, weo, wni, wno, fs, fr, hl, cs, cr)
    group = n_patch * n_sub
    n, d = nodes.shape
    e, c = edges.shape[0], ced.shape[0]
    halo = hl.shape[2]
    anywhere = pl.BlockSpec(memory_space=pl.ANY)
    inside = pl.BlockSpec(memory_space=pltpu.VMEM)
    dma = pltpu.SemaphoreType.DMA
    kept = [
        pltpu.VMEM((n, d), BF16),
        pltpu.VMEM((e, d), BF16),
        pltpu.VMEM((c, d), BF16),
        pltpu.VMEM((n, d), BF16),
        pltpu.VMEM((FIRST, d), F32),
        pltpu.VMEM((FIRST, d), F32),
        pltpu.VMEM(wni.shape, BF16),
        pltpu.VMEM(wno.shape, BF16),
    ]
    scratch = [pltpu.VMEM(x.shape, x.dtype) for x in (edges, ced, wei, weo, fs, fr, hl, cs, cr)] + [
        pltpu.VMEM((c, d), BF16),
        pltpu.VMEM((c, d), BF16),
        pltpu.VMEM(cs.shape, cs.dtype),
        pltpu.VMEM(cr.shape, cr.dtype),
        pltpu.VMEM((group, CO_DEV, d), BF16),
        pltpu.VMEM((group * CO_DEV, d), F32),
        pltpu.VMEM((2, halo, d), BF16),
        pltpu.VMEM((2, halo, d), BF16),
        pltpu.VMEM((group * CO_DEV, d), F32),
        pltpu.VMEM((group, CO_DEV, d), BF16),
        pltpu.VMEM((group // 2, CO_DEV, d), BF16),
        pltpu.VMEM((e, d), F32),
        dma((12,)), dma, dma, dma((2,)), dma((2,)), dma, dma, dma((3,)), dma((3,)), dma, dma,
        pltpu.SemaphoreType.REGULAR, pltpu.SemaphoreType.REGULAR,
    ]
    held = pl.pallas_call(
        functools.partial(kernel, n_patch, n_sub),
        out_shape=kept,
        in_specs=[anywhere] * len(operands),
        out_specs=[inside] * len(kept),
        scratch_shapes=scratch,
        compiler_params=pltpu.CompilerParams(
            collective_id=0, has_side_effects=True, vmem_limit_bytes=60 * 1024 * 1024),
        name="layer",
    )(*operands)
    return pl.pallas_call(
        finish,
        out_shape=[jax.ShapeDtypeStruct(x.shape, BF16) for x in (nodes, edges, ced)],
        in_specs=[inside] * len(kept),
        out_specs=[anywhere] * 3,
        scratch_shapes=[pltpu.VMEM((FIRST, d), BF16), dma((4,))],
        compiler_params=pltpu.CompilerParams(vmem_limit_bytes=8 * 1024 * 1024),
        name="finish",
    )(*held)


def solution(mesh):
    rows = P(("parts", "patch", "sub"), None)
    ids = P(("parts", "patch", "sub"))
    in_specs = (rows, rows, rows, P(), P(), P(), P(), ids, ids,
                P(("parts", "patch", "sub"), None, None), ids, ids)
    run = functools.partial(body, mesh.shape["patch"], mesh.shape["sub"])
    return jax.shard_map(run, mesh=mesh, in_specs=in_specs, out_specs=(rows, rows, rows),
                         check_vma=False)
```

```python
import functools

import jax
import jax.numpy as jnp
from jax import lax
from jax.experimental import pallas as pl
from jax.experimental.pallas import tpu as pltpu
from jax.sharding import PartitionSpec as P

CO_DEV = 4
FIRST = 16
F32 = jnp.float32
BF16 = jnp.bfloat16
MESH = pl.DeviceIdType.MESH


def dot(a, b, dims=((1,), (0,))):
    return lax.dot_general(a, b, (dims, ((), ())), preferred_element_type=F32)


def silu(v):
    half = 0.5 * v
    return (half + half * jnp.tanh(half)).astype(BF16)


def norm_rows(values):
    mean = jnp.mean(values, axis=-1, keepdims=True)
    centred = values - mean
    return centred * lax.rsqrt(jnp.mean(centred * centred, axis=-1, keepdims=True) + 1e-05)


def column(row):
    n = row.shape[1]
    wide = jnp.broadcast_to(row.astype(F32), (8, n))
    return jnp.transpose(wide)[:, :1]


def hot(col, first, count):
    lanes = lax.broadcasted_iota(jnp.int32, (col.shape[0], count), 1) + first
    return (col == lanes.astype(F32)).astype(BF16)


def hot_t(row, count):
    rows = lax.broadcasted_iota(jnp.int32, (count, row.shape[1]), 0)
    return (rows == row).astype(BF16)


def each(count, step):
    if count <= 16:
        for i in range(count):
            step(i)
    else:
        def run(i, carry):
            step(i)
            return carry

        lax.fori_loop(0, count, run, 0)


def node_rows(rows, pre, w_out):
    return (rows.astype(F32) + norm_rows(dot(silu(pre), w_out))).astype(BF16)


def kernel(
    n_patch, n_sub,
    nodes_h, edges_h, ced_h, wei_h, weo_h, wni_h, wno_h, fs_h, fr_h, hl_h, cs_h, cr_h,
    n_rows, ne_v, nc_v, nodes_v, n_pre, top, wni_v, wno_v,
    edges_v, ced_v, wei_v, weo_v, fs_v, fr_v, hl_v, cs_v, cr_v,
    mate_v, mate_new, mate_cs, mate_cr,
    heads_r, heads_f, halo_s, halo_r, part_f, part_s, part_r,
    acc, in_sem, ag_s, ag_r, halo_ss, halo_rs, rs_s, rs_r, mate_s, mate_r, back_s, back_r, near, go,
):
    group, shift = n_patch * n_sub, n_sub
    hubs = group - shift
    mp, ms = lax.axis_index("patch"), lax.axis_index("sub")
    me = mp * n_sub + ms
    hub, leaf = me < hubs, me >= hubs
    hosts = (me >= hubs - shift) & hub
    nodes_n, d = nodes_v.shape
    edges_n = edges_v.shape[0]
    halo = halo_s.shape[1]
    co = heads_r.shape[1]
    count = ced_v.shape[0]

    def rows_of(i):
        start = i * 2 * co
        return pl.ds(start if isinstance(i, int) else pl.multiple_of(start, 2 * co), 2 * co)

    def turn(i, by, n):
        at = i + by
        return jnp.where(at >= n, at - n, at)

    def device(i):
        if isinstance(i, int):
            at = {"patch": i // n_sub, "sub": i % n_sub}
        else:
            at = {"patch": lax.div(i, n_sub), "sub": lax.rem(i, n_sub)}
        return {"device_id": at, "device_id_type": MESH}

    def others(count, step):
        each(count, lambda i: pl.when(i != me)(lambda: step(i)))

    def await_rows(number, sem):
        span = heads_r.at[pl.ds(0, number)]
        pltpu.make_async_copy(span, span, sem).wait()

    barrier = pltpu.get_barrier_semaphore()

    @pl.when(hub)
    def _():
        others(group, lambda i: pl.semaphore_signal(barrier, inc=1, **device(i)))

    row = nodes_h.at[pl.ds(0, co)]

    def send_head(i):
        pltpu.make_async_remote_copy(
            src_ref=row, dst_ref=heads_r.at[me], send_sem=ag_s, recv_sem=ag_r,
            **device(i)).start()

    visit = [
        pltpu.make_async_remote_copy(
            src_ref=src, dst_ref=dst, send_sem=mate_s.at[i], recv_sem=mate_r.at[i],
            **device(me - shift))
        for i, (src, dst) in enumerate(((cs_h, mate_cs), (cr_h, mate_cr), (ced_h, mate_v)))
    ]
    back = pltpu.make_async_remote_copy(
        src_ref=mate_new, dst_ref=mate_v, send_sem=back_s, recv_sem=back_r, **device(me + shift))

    def away(i):
        return jnp.where(i >= hubs, 1, 0)

    prev, after = turn(me, group - 1, group), turn(me, 1, group)
    callers = away(prev) + away(after) + jnp.where(
        hosts, 1 + away(me + shift - 1) + away(turn(me + shift, 1, group)), 0)

    @pl.when(leaf)
    def _():
        pl.semaphore_wait(barrier, hubs)
        each(hubs, lambda i: send_head(hubs - 1 - i))
        for copy in visit:
            copy.start()
        pl.semaphore_signal(near, inc=1, **device(me - shift))
        for beside in (prev, after):
            pl.semaphore_signal(near, inc=1, **device(beside - shift * away(beside)))

    pairs = [
        (nodes_h, nodes_v), (hl_h, hl_v), (fs_h, fs_v), (fr_h, fr_v), (cs_h, cs_v), (cr_h, cr_v),
        (wei_h, wei_v), (edges_h, edges_v), (ced_h, ced_v),
        (weo_h, weo_v), (wni_h, wni_v), (wno_h, wno_v),
    ]
    loads = [pltpu.make_async_copy(h, v, in_sem.at[i]) for i, (h, v) in enumerate(pairs)]
    for copy in loads:
        copy.start()
    (l_nodes, l_hl, l_fs, l_fr, l_cs, l_cr, l_wei, l_edges, l_ced, l_weo, l_wni, l_wno) = loads

    l_nodes.wait()
    nodes = nodes_v[...]
    l_hl.wait()
    for side in range(2):
        pick = hot_t(hl_v[0, side:side + 1, :], nodes_n)
        halo_s[side] = dot(pick, nodes, ((0,), (0,))).astype(BF16)

    @pl.when(hub)
    def _():
        heads_r[me] = nodes_v[:co]
        pl.semaphore_wait(barrier, hubs - 1)
        each(hubs, lambda i: pl.when(hubs - 1 - i != me)(lambda: send_head(hubs - 1 - i)))

    halos, soon = [], []
    for side, to in ((0, after), (1, prev)):
        soon.append(to < hubs)
        halos.append(pltpu.make_async_remote_copy(
            src_ref=halo_s.at[side], dst_ref=halo_r.at[side],
            send_sem=halo_ss.at[side], recv_sem=halo_rs.at[side], **device(to)))
        pl.when(soon[-1])(halos[-1].start)

    l_fs.wait()
    l_fr.wait()
    l_cs.wait()
    l_cr.wait()
    fs, fr = fs_v[...], fr_v[...]
    fs_col = column(jnp.where(fs < halo, fs + (nodes_n + halo), fs - halo))
    fr_col = column(fr)

    l_wei.wait()
    own = jnp.concatenate(
        [dot(nodes, wei_v[d:2 * d]).astype(BF16), dot(nodes, wei_v[2 * d:]).astype(BF16)], axis=0)
    sel = jnp.concatenate([hot(fs_col, 0, nodes_n), hot(fr_col, 0, nodes_n)], axis=1)
    l_edges.wait()
    l_ced.wait()
    acc[...] = dot(edges_v[...], wei_v[:d]) + dot(sel, own)
    l_weo.wait()
    l_wni.wait()
    l_wno.wait()

    pl.when(hub & (callers > 0))(lambda: pl.semaphore_wait(near, callers))
    pl.when(hosts)(lambda: pl.semaphore_signal(go, inc=1, **device(me + shift)))
    pl.when(leaf)(lambda: pl.semaphore_wait(go, 1))
    for early, copy in zip(soon, halos):
        pl.when(jnp.logical_not(early))(copy.start)

    def coarse(hosting):
        ced, cs, cr = ced_v[...], cs_v[...], cr_v[...]
        ced_pre = dot(ced, wei_v[:d])
        if hosting:
            visit[0].wait_recv()
            visit[1].wait_recv()
            cs = jnp.concatenate([cs, mate_cs[...]], axis=1)
            cr = jnp.concatenate([cr, mate_cr[...]], axis=1)
        rows = cs.shape[1]
        picks = hot_t(cr, group * co)
        ends = jnp.concatenate(
            [hot(column(cs), 0, group * co), hot(column(cr), 0, group * co)], axis=0)
        if hosting:
            visit[2].wait_recv()
            ced_pre = jnp.concatenate([ced_pre, dot(mate_v[...], wei_v[:d])], axis=0)
            ced = jnp.concatenate([ced, mate_v[...]], axis=0)

        await_rows(group - 1, ag_r)

        def flat(i):
            both = jnp.concatenate(
                [heads_r[2 * i].astype(F32), heads_r[2 * i + 1].astype(F32)], axis=0)
            heads_f[rows_of(i), :] = both

        each(group // 2, flat)
        heads = heads_f[...].astype(BF16)
        c_ends = dot(ends, heads).astype(BF16)
        c_in = jnp.concatenate([c_ends[:rows], c_ends[rows:]], axis=1)
        c_hid = silu(ced_pre + dot(c_in, wei_v[d:]))
        c_new = (ced.astype(F32) + norm_rows(dot(c_hid, weo_v[...]))).astype(BF16)
        part_f[...] = dot(picks, c_new)

        def send_part(i):
            pltpu.make_async_remote_copy(
                src_ref=part_s.at[i], dst_ref=part_r.at[me],
                send_sem=rs_s, recv_sem=rs_r, **device(i)).start()

        def pack(i):
            both = part_f[rows_of(i), :].astype(BF16)
            for j in range(2):
                at = 2 * i + j
                part_s[at] = both[j * co:(j + 1) * co]
                pl.when(me != at)(lambda: send_part(at))

        each(group // 2, pack)
        if hosting:
            mate_new[...] = c_new[count:]
            back.start()
        part_r[me] = part_s[me]
        nc_v[...] = c_new[:count]

    pl.when(hub & jnp.logical_not(hosts))(lambda: coarse(False))
    pl.when(hosts)(lambda: coarse(True))

    for copy in halos:
        copy.wait_recv()
    far = dot(jnp.concatenate([halo_r[1], halo_r[0]], axis=0), wei_v[d:2 * d]).astype(BF16)
    hid = silu(acc[...] + dot(hot(fs_col, nodes_n, 2 * halo), far))
    delta = norm_rows(dot(hid, weo_v[...]))
    e_new = (edges_v[...].astype(F32) + jnp.where(fr_col >= 0.0, delta, 0.0)).astype(BF16)
    ne_v[...] = e_new
    fine = dot(hot_t(fr, nodes_n), e_new)

    pre = dot(nodes, wni_v[:d])
    n_rows[...] = node_rows(nodes, pre + dot(fine.astype(BF16), wni_v[d:]), wno_v[...])
    first = top.shape[0]
    n_pre[...] = pre[:first]
    top[...] = fine[:first]

    for copy in halos:
        copy.wait_send()

    pl.when(hosts)(back.wait_send)

    @pl.when(hub)
    def _():
        await_rows(hubs - 1, ag_s)
        await_rows(group - 1, rs_s)
        await_rows(hubs - 1, rs_r)

    @pl.when(leaf)
    def _():
        await_rows(hubs, ag_s)
        for copy in visit:
            copy.wait_send()
        back.wait_recv()
        nc_v[...] = mate_v[...]
        await_rows(hubs, rs_r)

    top[:co] += jnp.sum(part_r[...].astype(F32), axis=0)


def finish(n_rows, ne_v, nc_v, nodes_v, n_pre, top, wni_v, wno_v, nn_h, ne_h, nc_h, first_v, sem):
    first, d = top.shape
    n = n_rows.shape[0]
    copies = [
        pltpu.make_async_copy(ne_v, ne_h, sem.at[0]),
        pltpu.make_async_copy(nc_v, nc_h, sem.at[1]),
        pltpu.make_async_copy(n_rows.at[pl.ds(first, n - first)], nn_h.at[pl.ds(first, n - first)],
                              sem.at[2]),
    ]
    for copy in copies:
        copy.start()
    pre = n_pre[...] + dot(top[...].astype(BF16), wni_v[d:])
    first_v[...] = node_rows(nodes_v[:first], pre, wno_v[...])
    copies.append(pltpu.make_async_copy(first_v, nn_h.at[pl.ds(0, first)], sem.at[3]))
    copies[-1].start()
    for copy in copies:
        copy.wait()


def body(n_patch, n_sub, *args):
    nodes, edges, ced, wei, weo, wni, wno, fs, fr, hl, cs, cr = args
    fs, fr, cs, cr = (x.reshape(1, -1) for x in (fs, fr, cs, cr))
    operands = (nodes, edges, ced, wei, weo, wni, wno, fs, fr, hl, cs, cr)
    group = n_patch * n_sub
    n, d = nodes.shape
    e, c = edges.shape[0], ced.shape[0]
    halo = hl.shape[2]
    anywhere = pl.BlockSpec(memory_space=pl.ANY)
    inside = pl.BlockSpec(memory_space=pltpu.VMEM)
    dma = pltpu.SemaphoreType.DMA
    kept = [
        pltpu.VMEM((n, d), BF16),
        pltpu.VMEM((e, d), BF16),
        pltpu.VMEM((c, d), BF16),
        pltpu.VMEM((n, d), BF16),
        pltpu.VMEM((FIRST, d), F32),
        pltpu.VMEM((FIRST, d), F32),
        pltpu.VMEM(wni.shape, BF16),
        pltpu.VMEM(wno.shape, BF16),
    ]
    scratch = [pltpu.VMEM(x.shape, x.dtype) for x in (edges, ced, wei, weo, fs, fr, hl, cs, cr)] + [
        pltpu.VMEM((c, d), BF16),
        pltpu.VMEM((c, d), BF16),
        pltpu.VMEM(cs.shape, cs.dtype),
        pltpu.VMEM(cr.shape, cr.dtype),
        pltpu.VMEM((group, CO_DEV, d), BF16),
        pltpu.VMEM((group * CO_DEV, d), F32),
        pltpu.VMEM((2, halo, d), BF16),
        pltpu.VMEM((2, halo, d), BF16),
        pltpu.VMEM((group * CO_DEV, d), F32),
        pltpu.VMEM((group, CO_DEV, d), BF16),
        pltpu.VMEM((group - n_sub, CO_DEV, d), BF16),
        pltpu.VMEM((e, d), F32),
        dma((12,)), dma, dma, dma((2,)), dma((2,)), dma, dma, dma((3,)), dma((3,)), dma, dma,
        pltpu.SemaphoreType.REGULAR, pltpu.SemaphoreType.REGULAR,
    ]
    held = pl.pallas_call(
        functools.partial(kernel, n_patch, n_sub),
        out_shape=kept,
        in_specs=[anywhere] * len(operands),
        out_specs=[inside] * len(kept),
        scratch_shapes=scratch,
        compiler_params=pltpu.CompilerParams(
            collective_id=0, has_side_effects=True, vmem_limit_bytes=60 * 1024 * 1024),
        name="layer",
    )(*operands)
    return pl.pallas_call(
        finish,
        out_shape=[jax.ShapeDtypeStruct(x.shape, BF16) for x in (nodes, edges, ced)],
        in_specs=[inside] * len(kept),
        out_specs=[anywhere] * 3,
        scratch_shapes=[pltpu.VMEM((FIRST, d), BF16), dma((4,))],
        compiler_params=pltpu.CompilerParams(vmem_limit_bytes=8 * 1024 * 1024),
        name="finish",
    )(*held)


def solution(mesh):
    rows = P(("parts", "patch", "sub"), None)
    ids = P(("parts", "patch", "sub"))
    in_specs = (rows, rows, rows, P(), P(), P(), P(), ids, ids,
                P(("parts", "patch", "sub"), None, None), ids, ids)
    run = functools.partial(body, mesh.shape["patch"], mesh.shape["sub"])
    return jax.shard_map(run, mesh=mesh, in_specs=in_specs, out_specs=(rows, rows, rows),
                         check_vma=False)
```

```python
import functools

import jax
import jax.numpy as jnp
from jax import lax
from jax.experimental import pallas as pl
from jax.experimental.pallas import tpu as pltpu
from jax.sharding import PartitionSpec as P

CO_DEV = 4
FIRST = 16
F32 = jnp.float32
BF16 = jnp.bfloat16
MESH = pl.DeviceIdType.MESH


def dot(a, b, dims=((1,), (0,))):
    return lax.dot_general(a, b, (dims, ((), ())), preferred_element_type=F32)


def silu(v):
    half = 0.5 * v
    return (half + half * jnp.tanh(half)).astype(BF16)


def norm_rows(values):
    mean = jnp.mean(values, axis=-1, keepdims=True)
    centred = values - mean
    return centred * lax.rsqrt(jnp.mean(centred * centred, axis=-1, keepdims=True) + 1e-05)


def column(row):
    n = row.shape[1]
    wide = jnp.broadcast_to(row.astype(F32), (8, n))
    return jnp.transpose(wide)[:, :1]


def hot(col, first, count):
    lanes = lax.broadcasted_iota(jnp.int32, (col.shape[0], count), 1) + first
    return (col == lanes.astype(F32)).astype(BF16)


def hot_t(row, count):
    rows = lax.broadcasted_iota(jnp.int32, (count, row.shape[1]), 0)
    return (rows == row).astype(BF16)


def each(count, step):
    if count <= 16:
        for i in range(count):
            step(i)
    else:
        def run(i, carry):
            step(i)
            return carry

        lax.fori_loop(0, count, run, 0)


def node_rows(rows, pre, w_out):
    return (rows.astype(F32) + norm_rows(dot(silu(pre), w_out))).astype(BF16)


def kernel(
    n_patch, n_sub,
    nodes_h, edges_h, ced_h, wei_h, weo_h, wni_h, wno_h, fs_h, fr_h, hl_h, cs_h, cr_h,
    n_rows, ne_v, nc_v, nodes_v, n_pre, top, wni_v, wno_v,
    edges_v, ced_v, wei_v, weo_v, fs_v, fr_v, hl_v, cs_v, cr_v,
    mate_v, mate_new, mate_ids,
    heads_r, heads_f, halo_s, halo_r, part_f, part_s, part_r,
    acc, in_sem, sent, ag_s, ag_r, halo_rs, rs_s, rs_r, ids_r, mate_r, near,
):
    group, shift = n_patch * n_sub, n_sub
    hub_p = n_patch - 1
    hubs = group - shift
    mp, ms = lax.axis_index("patch"), lax.axis_index("sub")
    me = mp * n_sub + ms
    hub, leaf, hosts = mp < hub_p, mp == hub_p, mp == hub_p - 1
    nodes_n, d = nodes_v.shape
    halo = halo_s.shape[1]
    co = heads_r.shape[1]
    count = ced_v.shape[0]

    def rows_of(i):
        start = i * 2 * co
        return pl.ds(start if isinstance(i, int) else pl.multiple_of(start, 2 * co), 2 * co)

    def turn(i, by, n):
        at = i + by
        return jnp.where(at >= n, at - n, at)

    def device(p, s):
        return {"device_id": {"patch": p, "sub": s}, "device_id_type": MESH}

    def device_of(i):
        if isinstance(i, int):
            return device(i // n_sub, i % n_sub)
        return device(lax.div(i, n_sub), lax.rem(i, n_sub))

    subs = [ms] + [turn(ms, j, n_sub) for j in range(1, n_sub)]

    def patch(p, step):
        for s in subs:
            step(p, s)

    def beside(step):
        for s in subs[1:]:
            step(mp, s)

    def await_rows(number, sem):
        span = heads_r.at[pl.ds(0, number)]
        pltpu.make_async_copy(span, span, sem).wait()

    barrier = pltpu.get_barrier_semaphore()

    def hail(p, s):
        pl.semaphore_signal(barrier, inc=1, **device(p, s))

    host, guest = device(mp - 1, ms), device(mp + 1, ms)
    visit = [
        pltpu.make_async_remote_copy(
            src_ref=src, dst_ref=dst, send_sem=out, recv_sem=sem, **host)
        for src, dst, out, sem in (
            (ced_h, mate_v, sent, mate_r),
            (cs_h, mate_ids.at[0], ids_r, ids_r), (cr_h, mate_ids.at[1], ids_r, ids_r))
    ]
    await_ids = pltpu.make_async_copy(mate_ids, mate_ids, ids_r).wait
    back = pltpu.make_async_remote_copy(
        src_ref=mate_new, dst_ref=mate_v, send_sem=sent, recv_sem=mate_r, **guest)

    @pl.when(hub)
    def _():
        pl.when(hosts)(lambda: hail(mp + 1, ms))
        each(hub_p - 1, lambda i: patch(turn(mp, i + 1, hub_p), hail))
        beside(hail)

    @pl.when(leaf)
    def _():
        pl.semaphore_wait(barrier, 1)
        for copy in visit:
            copy.start()

    groups = [
        [(nodes_h, nodes_v), (hl_h, hl_v)],
        [(fs_h, fs_v), (fr_h, fr_v), (cs_h, cs_v), (cr_h, cr_v), (wei_h, wei_v)],
        [(edges_h, edges_v), (ced_h, ced_v), (weo_h, weo_v), (wni_h, wni_v), (wno_h, wno_v)],
    ]
    loads = [[pltpu.make_async_copy(h, v, in_sem.at[i]) for h, v in pairs]
             for i, pairs in enumerate(groups)]
    for copies in loads:
        for copy in copies:
            copy.start()

    def loaded(i):
        for copy in loads[i]:
            copy.wait()

    loaded(0)
    nodes = nodes_v[...]
    head_row = heads_r.at[me]

    def send_head(p, s):
        pltpu.make_async_remote_copy(
            src_ref=head_row, dst_ref=head_row, send_sem=ag_s, recv_sem=ag_r,
            **device(p, s)).start()

    heads_r[me] = nodes[:co]

    @pl.when(hub)
    def _():
        pl.semaphore_wait(barrier, hubs - 1)
        pl.when(hosts)(lambda: hail(mp + 1, ms))
        each(hub_p - 1, lambda i: patch(turn(mp, hub_p - 1 - i, hub_p), send_head))
        beside(send_head)

    for side in range(2):
        pick = hot_t(hl_v[0, side:side + 1, :], nodes_n)
        halo_s[side] = dot(pick, nodes, ((0,), (0,))).astype(BF16)

    prev, after = turn(me, group - 1, group), turn(me, 1, group)

    def away(i):
        return jnp.where(i >= hubs, 1, 0)

    @pl.when(leaf)
    def _():
        pl.semaphore_wait(barrier, 1)
        each(hub_p, lambda i: patch(hub_p - 1 - i, send_head))
        pl.semaphore_signal(near, inc=1, **host)
        for i in (prev, after):
            pl.semaphore_signal(near, inc=1, **device_of(i - shift * away(i)))

    halos, soon = [], []
    for side, to in ((0, after), (1, prev)):
        soon.append(to < hubs)
        halos.append(pltpu.make_async_remote_copy(
            src_ref=halo_s.at[side], dst_ref=halo_r.at[side],
            send_sem=sent, recv_sem=halo_rs, **device_of(to)))
        pl.when(soon[-1])(halos[-1].start)

    loaded(1)
    fs, fr = fs_v[...], fr_v[...]
    fs_col = column(jnp.where(fs < halo, fs + (nodes_n + halo), fs - halo))
    fr_col = column(fr)
    own = jnp.concatenate(
        [dot(nodes, wei_v[d:2 * d]).astype(BF16), dot(nodes, wei_v[2 * d:]).astype(BF16)], axis=0)
    sel = jnp.concatenate([hot(fs_col, 0, nodes_n), hot(fr_col, 0, nodes_n)], axis=1)
    loaded(2)
    acc[...] = dot(edges_v[...], wei_v[:d]) + dot(sel, own)

    callers = away(prev) + away(after) + jnp.where(
        hosts, 1 + away(me + shift - 1) + away(turn(me + shift, 1, group)), 0)
    pl.when(hub & (callers > 0))(lambda: pl.semaphore_wait(near, callers))
    pl.when(hosts)(lambda: pl.semaphore_signal(near, inc=1, **guest))
    pl.when(leaf)(lambda: pl.semaphore_wait(near, 1))
    for early, copy in zip(soon, halos):
        pl.when(jnp.logical_not(early))(copy.start)

    def coarse(hosting):
        ced, cs, cr = ced_v[...], cs_v[...], cr_v[...]
        ced_pre = dot(ced, wei_v[:d])
        if hosting:
            await_ids()
            cs = jnp.concatenate([cs, mate_ids[0]], axis=1)
            cr = jnp.concatenate([cr, mate_ids[1]], axis=1)
        rows = cs.shape[1]
        picks = hot_t(cr, group * co)
        ends = jnp.concatenate(
            [hot(column(cs), 0, group * co), hot(column(cr), 0, group * co)], axis=0)
        if hosting:
            visit[0].wait_recv()
            ced_pre = jnp.concatenate([ced_pre, dot(mate_v[...], wei_v[:d])], axis=0)
            ced = jnp.concatenate([ced, mate_v[...]], axis=0)

        await_rows(group - 1, ag_r)

        def flat(i):
            both = jnp.concatenate(
                [heads_r[2 * i].astype(F32), heads_r[2 * i + 1].astype(F32)], axis=0)
            heads_f[rows_of(i), :] = both

        each(group // 2, flat)
        heads = heads_f[...].astype(BF16)
        c_ends = dot(ends, heads).astype(BF16)
        c_in = jnp.concatenate([c_ends[:rows], c_ends[rows:]], axis=1)
        c_hid = silu(ced_pre + dot(c_in, wei_v[d:]))
        c_new = (ced.astype(F32) + norm_rows(dot(c_hid, weo_v[...]))).astype(BF16)
        part_f[...] = dot(picks, c_new)

        def send_part(i):
            pltpu.make_async_remote_copy(
                src_ref=part_s.at[i], dst_ref=part_r.at[me],
                send_sem=rs_s, recv_sem=rs_r, **device_of(i)).start()

        def pack(i):
            both = part_f[rows_of(i), :].astype(BF16)
            for j in range(2):
                at = 2 * i + j
                part_s[at] = both[j * co:(j + 1) * co]
                pl.when(me != at)(lambda: send_part(at))

        each(group // 2, pack)
        if hosting:
            mate_new[...] = c_new[count:]
            back.start()
        part_r[me] = part_s[me]
        nc_v[...] = c_new[:count]

    pl.when(hub & jnp.logical_not(hosts))(lambda: coarse(False))
    pl.when(hosts)(lambda: coarse(True))

    pltpu.make_async_copy(halo_r, halo_r, halo_rs).wait()
    far = dot(jnp.concatenate([halo_r[1], halo_r[0]], axis=0), wei_v[d:2 * d]).astype(BF16)
    hid = silu(acc[...] + dot(hot(fs_col, nodes_n, 2 * halo), far))
    delta = norm_rows(dot(hid, weo_v[...]))
    e_new = (edges_v[...].astype(F32) + jnp.where(fr_col >= 0.0, delta, 0.0)).astype(BF16)
    ne_v[...] = e_new
    fine = dot(hot_t(fr, nodes_n), e_new)

    pre = dot(nodes, wni_v[:d])
    n_rows[...] = node_rows(nodes, pre + dot(fine.astype(BF16), wni_v[d:]), wno_v[...])
    first = top.shape[0]
    n_pre[...] = pre[:first]
    top[...] = fine[:first]

    def await_sent(rows):
        span = edges_v.at[pl.ds(0, rows)]
        pltpu.make_async_copy(span, span, sent).wait()

    pl.when(mp < hub_p - 1)(lambda: await_sent(2 * halo))
    pl.when(mp >= hub_p - 1)(lambda: await_sent(2 * halo + count))

    @pl.when(hub)
    def _():
        await_rows(hubs - 1, ag_s)
        await_rows(group - 1, rs_s)
        await_rows(hubs - 1, rs_r)

    @pl.when(leaf)
    def _():
        await_rows(hubs, ag_s)
        await_ids()
        back.wait_recv()
        nc_v[...] = mate_v[...]
        await_rows(hubs, rs_r)

    top[:co] += jnp.sum(part_r[...].astype(F32), axis=0)


def finish(n_rows, ne_v, nc_v, nodes_v, n_pre, top, wni_v, wno_v, nn_h, ne_h, nc_h, first_v, sem):
    first, d = top.shape
    n = n_rows.shape[0]
    copies = [
        pltpu.make_async_copy(ne_v, ne_h, sem.at[0]),
        pltpu.make_async_copy(nc_v, nc_h, sem.at[1]),
        pltpu.make_async_copy(n_rows.at[pl.ds(first, n - first)], nn_h.at[pl.ds(first, n - first)],
                              sem.at[2]),
    ]
    for copy in copies:
        copy.start()
    pre = n_pre[...] + dot(top[...].astype(BF16), wni_v[d:])
    first_v[...] = node_rows(nodes_v[:first], pre, wno_v[...])
    copies.append(pltpu.make_async_copy(first_v, nn_h.at[pl.ds(0, first)], sem.at[3]))
    copies[-1].start()
    for copy in copies:
        copy.wait()


def body(n_patch, n_sub, *args):
    nodes, edges, ced, wei, weo, wni, wno, fs, fr, hl, cs, cr = args
    fs, fr, cs, cr = (x.reshape(1, -1) for x in (fs, fr, cs, cr))
    operands = (nodes, edges, ced, wei, weo, wni, wno, fs, fr, hl, cs, cr)
    group = n_patch * n_sub
    n, d = nodes.shape
    e, c = edges.shape[0], ced.shape[0]
    halo = hl.shape[2]
    anywhere = pl.BlockSpec(memory_space=pl.ANY)
    inside = pl.BlockSpec(memory_space=pltpu.VMEM)
    dma = pltpu.SemaphoreType.DMA
    kept = [
        pltpu.VMEM((n, d), BF16),
        pltpu.VMEM((e, d), BF16),
        pltpu.VMEM((c, d), BF16),
        pltpu.VMEM((n, d), BF16),
        pltpu.VMEM((FIRST, d), F32),
        pltpu.VMEM((FIRST, d), F32),
        pltpu.VMEM(wni.shape, BF16),
        pltpu.VMEM(wno.shape, BF16),
    ]
    scratch = [pltpu.VMEM(x.shape, x.dtype) for x in (edges, ced, wei, weo, fs, fr, hl, cs, cr)] + [
        pltpu.VMEM((c, d), BF16),
        pltpu.VMEM((c, d), BF16),
        pltpu.VMEM((2,) + cs.shape, cs.dtype),
        pltpu.VMEM((group, CO_DEV, d), BF16),
        pltpu.VMEM((group * CO_DEV, d), F32),
        pltpu.VMEM((2, halo, d), BF16),
        pltpu.VMEM((2, halo, d), BF16),
        pltpu.VMEM((group * CO_DEV, d), F32),
        pltpu.VMEM((group, CO_DEV, d), BF16),
        pltpu.VMEM((group - n_sub, CO_DEV, d), BF16),
        pltpu.VMEM((e, d), F32),
        dma((3,)), dma, dma, dma, dma, dma, dma, dma, dma, pltpu.SemaphoreType.REGULAR,
    ]
    held = pl.pallas_call(
        functools.partial(kernel, n_patch, n_sub),
        out_shape=kept,
        in_specs=[anywhere] * len(operands),
        out_specs=[inside] * len(kept),
        scratch_shapes=scratch,
        compiler_params=pltpu.CompilerParams(
            collective_id=0, has_side_effects=True, vmem_limit_bytes=60 * 1024 * 1024),
        name="layer",
    )(*operands)
    return pl.pallas_call(
        finish,
        out_shape=[jax.ShapeDtypeStruct(x.shape, BF16) for x in (nodes, edges, ced)],
        in_specs=[inside] * len(kept),
        out_specs=[anywhere] * 3,
        scratch_shapes=[pltpu.VMEM((FIRST, d), BF16), dma((4,))],
        compiler_params=pltpu.CompilerParams(vmem_limit_bytes=8 * 1024 * 1024),
        name="finish",
    )(*held)


def solution(mesh):
    rows = P(("parts", "patch", "sub"), None)
    ids = P(("parts", "patch", "sub"))
    in_specs = (rows, rows, rows, P(), P(), P(), P(), ids, ids,
                P(("parts", "patch", "sub"), None, None), ids, ids)
    run = functools.partial(body, mesh.shape["patch"], mesh.shape["sub"])
    return jax.shard_map(run, mesh=mesh, in_specs=in_specs, out_specs=(rows, rows, rows),
                         check_vma=False)
```

```python
import functools

import jax
import jax.numpy as jnp
from jax import lax
from jax.experimental import pallas as pl
from jax.experimental.pallas import tpu as pltpu
from jax.sharding import PartitionSpec as P

CO_DEV = 4
FIRST = 16
F32 = jnp.float32
BF16 = jnp.bfloat16
MESH = pl.DeviceIdType.MESH


def dot(a, b, dims=((1,), (0,))):
    return lax.dot_general(a, b, (dims, ((), ())), preferred_element_type=F32)


def silu(v):
    half = 0.5 * v
    return (half + half * jnp.tanh(half)).astype(BF16)


def norm_rows(values):
    mean = jnp.mean(values, axis=-1, keepdims=True)
    centred = values - mean
    return centred * lax.rsqrt(jnp.mean(centred * centred, axis=-1, keepdims=True) + 1e-05)


def column(row):
    n = row.shape[1]
    wide = jnp.broadcast_to(row.astype(F32), (8, n))
    return jnp.transpose(wide)[:, :1]


def hot(col, first, count):
    lanes = lax.broadcasted_iota(jnp.int32, (col.shape[0], count), 1) + first
    return (col == lanes.astype(F32)).astype(BF16)


def hot_t(row, count):
    rows = lax.broadcasted_iota(jnp.int32, (count, row.shape[1]), 0)
    return (rows == row).astype(BF16)


def each(count, step):
    if count <= 16:
        for i in range(count):
            step(i)
    else:
        def run(i, carry):
            step(i)
            return carry

        lax.fori_loop(0, count, run, 0)


def node_rows(rows, pre, w_out):
    return (rows.astype(F32) + norm_rows(dot(silu(pre), w_out))).astype(BF16)


def kernel(
    n_patch, n_sub,
    nodes_h, edges_h, ced_h, wei_h, weo_h, wni_h, wno_h, fs_h, fr_h, hl_h, cs_h, cr_h,
    n_rows, ne_v, nc_v, nodes_v, n_pre, top, wni_v, wno_v,
    edges_v, ced_v, wei_v, weo_v, fs_v, fr_v, hl_v, cs_v, cr_v,
    mate_v, mate_new, mate_ids,
    heads_r, heads_f, halo_s, halo_r, part_f, part_s, part_r,
    acc, ced_pre, in_sem, sent, ag_s, ag_r, halo_rs, rs_s, rs_r, ids_r, mate_r, near,
):
    group, shift = n_patch * n_sub, n_sub
    hub_p = n_patch - 1
    hubs = group - shift
    mp, ms = lax.axis_index("patch"), lax.axis_index("sub")
    me = mp * n_sub + ms
    hub, leaf, hosts = mp < hub_p, mp == hub_p, mp == hub_p - 1
    nodes_n, d = nodes_v.shape
    halo = halo_s.shape[1]
    co = heads_r.shape[1]
    count = ced_v.shape[0]

    def rows_of(i):
        start = i * 2 * co
        return pl.ds(start if isinstance(i, int) else pl.multiple_of(start, 2 * co), 2 * co)

    def turn(i, by, n):
        at = i + by
        return jnp.where(at >= n, at - n, at)

    def device(p, s):
        return {"device_id": {"patch": p, "sub": s}, "device_id_type": MESH}

    def device_of(i):
        if isinstance(i, int):
            return device(i // n_sub, i % n_sub)
        return device(lax.div(i, n_sub), lax.rem(i, n_sub))

    subs = [turn(ms, j, n_sub) for j in list(range(n_sub // 2, n_sub)) + list(range(1, n_sub // 2))]

    def patch(p, step):
        for s in subs + [ms]:
            step(p, s)

    def beside(step):
        for s in subs:
            step(mp, s)

    def await_rows(number, sem):
        span = heads_r.at[pl.ds(0, number)]
        pltpu.make_async_copy(span, span, sem).wait()

    barrier = pltpu.get_barrier_semaphore()

    def hail(p, s):
        pl.semaphore_signal(barrier, inc=1, **device(p, s))

    host, guest = device(mp - 1, ms), device(mp + 1, ms)
    visit = [
        pltpu.make_async_remote_copy(
            src_ref=src, dst_ref=dst, send_sem=out, recv_sem=sem, **host)
        for src, dst, out, sem in (
            (ced_h, mate_v, sent, mate_r),
            (cs_h, mate_ids.at[0], ids_r, ids_r), (cr_h, mate_ids.at[1], ids_r, ids_r))
    ]
    await_ids = pltpu.make_async_copy(mate_ids, mate_ids, ids_r).wait
    back = pltpu.make_async_remote_copy(
        src_ref=mate_new, dst_ref=mate_v, send_sem=sent, recv_sem=mate_r, **guest)

    @pl.when(hub)
    def _():
        patch(turn(mp, 1, hub_p), hail)
        pl.when(hosts)(lambda: hail(mp + 1, ms))
        each(hub_p - 2, lambda i: patch(turn(mp, i + 2, hub_p), hail))
        beside(hail)

    @pl.when(leaf)
    def _():
        pl.semaphore_wait(barrier, 1)
        for copy in visit:
            copy.start()

    groups = [
        [(nodes_h, nodes_v), (hl_h, hl_v)],
        [(fs_h, fs_v), (fr_h, fr_v), (cs_h, cs_v), (cr_h, cr_v), (wei_h, wei_v)],
        [(edges_h, edges_v), (ced_h, ced_v), (weo_h, weo_v), (wni_h, wni_v), (wno_h, wno_v)],
    ]
    loads = [[pltpu.make_async_copy(h, v, in_sem.at[i]) for h, v in pairs]
             for i, pairs in enumerate(groups)]
    for copies in loads:
        for copy in copies:
            copy.start()

    def loaded(i):
        for copy in loads[i]:
            copy.wait()

    loaded(0)
    nodes = nodes_v[...]
    head_row = heads_r.at[me]

    def send_head(p, s):
        pltpu.make_async_remote_copy(
            src_ref=head_row, dst_ref=head_row, send_sem=ag_s, recv_sem=ag_r,
            **device(p, s)).start()

    heads_r[me] = nodes[:co]

    @pl.when(hub)
    def _():
        pl.semaphore_wait(barrier, hubs - 1)
        pl.when(hosts)(lambda: hail(mp + 1, ms))
        each(hub_p - 1, lambda i: patch(turn(mp, hub_p - 1 - i, hub_p), send_head))
        beside(send_head)

    prev, after = turn(me, group - 1, group), turn(me, 1, group)

    def away(i):
        return jnp.where(i >= hubs, 1, 0)

    @pl.when(leaf)
    def _():
        pl.semaphore_wait(barrier, 1)
        each(hub_p, lambda i: patch(hub_p - 1 - i, send_head))
        pl.semaphore_signal(near, inc=1, **host)
        for i in (prev, after):
            pl.semaphore_signal(near, inc=1, **device_of(i - shift * away(i)))

    for side in range(2):
        pick = hot_t(hl_v[0, side:side + 1, :], nodes_n)
        halo_s[side] = dot(pick, nodes, ((0,), (0,))).astype(BF16)

    halos, soon = [], []
    for side, to in ((0, after), (1, prev)):
        soon.append(to < hubs)
        halos.append(pltpu.make_async_remote_copy(
            src_ref=halo_s.at[side], dst_ref=halo_r.at[side],
            send_sem=sent, recv_sem=halo_rs, **device_of(to)))
        pl.when(soon[-1])(halos[-1].start)

    loaded(1)
    fs, fr = fs_v[...], fr_v[...]
    fs_col = column(jnp.where(fs < halo, fs + (nodes_n + halo), fs - halo))
    fr_col = column(fr)
    own = jnp.concatenate(
        [dot(nodes, wei_v[d:2 * d]).astype(BF16), dot(nodes, wei_v[2 * d:]).astype(BF16)], axis=0)
    sel = jnp.concatenate([hot(fs_col, 0, nodes_n), hot(fr_col, 0, nodes_n)], axis=1)
    loaded(2)
    acc[...] = dot(edges_v[...], wei_v[:d]) + dot(sel, own)

    callers = away(prev) + away(after) + jnp.where(
        hosts, 1 + away(me + shift - 1) + away(turn(me + shift, 1, group)), 0)
    pl.when(hub & (callers > 0))(lambda: pl.semaphore_wait(near, callers))
    pl.when(hosts)(lambda: pl.semaphore_signal(near, inc=1, **guest))
    pl.when(leaf)(lambda: pl.semaphore_wait(near, 1))
    for early, copy in zip(soon, halos):
        pl.when(jnp.logical_not(early))(copy.start)

    def coarse(hosting):
        ced, cs, cr = ced_v[...], cs_v[...], cr_v[...]
        ced_pre[:count] = dot(ced, wei_v[:d])
        if hosting:
            await_ids()
            cs = jnp.concatenate([cs, mate_ids[0]], axis=1)
            cr = jnp.concatenate([cr, mate_ids[1]], axis=1)
        rows = cs.shape[1]
        picks = hot_t(cr, group * co)
        ends = jnp.concatenate(
            [hot(column(cs), 0, group * co), hot(column(cr), 0, group * co)], axis=0)
        if hosting:
            visit[0].wait_recv()
            ced_pre[count:] = dot(mate_v[...], wei_v[:d])
            ced = jnp.concatenate([ced, mate_v[...]], axis=0)

        await_rows(group - 1, ag_r)

        def flat(i):
            both = jnp.concatenate(
                [heads_r[2 * i].astype(F32), heads_r[2 * i + 1].astype(F32)], axis=0)
            heads_f[rows_of(i), :] = both

        each(group // 2, flat)
        heads = heads_f[...].astype(BF16)
        c_ends = dot(ends, heads).astype(BF16)
        c_in = jnp.concatenate([c_ends[:rows], c_ends[rows:]], axis=1)
        c_hid = silu(ced_pre[:rows] + dot(c_in, wei_v[d:]))
        c_new = (ced.astype(F32) + norm_rows(dot(c_hid, weo_v[...]))).astype(BF16)
        part_f[...] = dot(picks, c_new)

        def send_part(i):
            pltpu.make_async_remote_copy(
                src_ref=part_s.at[i], dst_ref=part_r.at[me],
                send_sem=rs_s, recv_sem=rs_r, **device_of(i)).start()

        def pack(i):
            both = part_f[rows_of(i), :].astype(BF16)
            for j in range(2):
                at = 2 * i + j
                part_s[at] = both[j * co:(j + 1) * co]
                pl.when(me != at)(lambda: send_part(at))

        each(group // 2, pack)
        if hosting:
            mate_new[...] = c_new[count:]
            back.start()
        part_r[me] = part_s[me]
        nc_v[...] = c_new[:count]

    pl.when(hub & jnp.logical_not(hosts))(lambda: coarse(False))
    pl.when(hosts)(lambda: coarse(True))

    pltpu.make_async_copy(halo_r, halo_r, halo_rs).wait()
    far = dot(jnp.concatenate([halo_r[1], halo_r[0]], axis=0), wei_v[d:2 * d]).astype(BF16)
    hid = silu(acc[...] + dot(hot(fs_col, nodes_n, 2 * halo), far))
    delta = norm_rows(dot(hid, weo_v[...]))
    e_new = (edges_v[...].astype(F32) + jnp.where(fr_col >= 0.0, delta, 0.0)).astype(BF16)
    ne_v[...] = e_new
    fine = dot(hot_t(fr, nodes_n), e_new)

    pre = dot(nodes, wni_v[:d])
    n_rows[...] = node_rows(nodes, pre + dot(fine.astype(BF16), wni_v[d:]), wno_v[...])
    first = top.shape[0]
    n_pre[...] = pre[:first]
    top[...] = fine[:first]

    def await_sent(rows):
        span = edges_v.at[pl.ds(0, rows)]
        pltpu.make_async_copy(span, span, sent).wait()

    pl.when(mp < hub_p - 1)(lambda: await_sent(2 * halo))
    pl.when(mp >= hub_p - 1)(lambda: await_sent(2 * halo + count))

    @pl.when(hub)
    def _():
        await_rows(hubs - 1, ag_s)
        await_rows(group - 1, rs_s)
        await_rows(hubs - 1, rs_r)

    @pl.when(leaf)
    def _():
        await_rows(hubs, ag_s)
        await_ids()
        back.wait_recv()
        nc_v[...] = mate_v[...]
        await_rows(hubs, rs_r)

    top[:co] += jnp.sum(part_r[...].astype(F32), axis=0)


def finish(n_rows, ne_v, nc_v, nodes_v, n_pre, top, wni_v, wno_v, nn_h, ne_h, nc_h, first_v, sem):
    first, d = top.shape
    n = n_rows.shape[0]
    for src, dst in (
            (ne_v, ne_h), (nc_v, nc_h),
            (n_rows.at[pl.ds(first, n - first)], nn_h.at[pl.ds(first, n - first)])):
        pltpu.make_async_copy(src, dst, sem).start()
    pre = n_pre[...] + dot(top[...].astype(BF16), wni_v[d:])
    first_v[...] = node_rows(nodes_v[:first], pre, wno_v[...])
    pltpu.make_async_copy(first_v, nn_h.at[pl.ds(0, first)], sem).start()
    span = wni_v.at[pl.ds(0, ne_v.shape[0] + nc_v.shape[0] + n)]
    pltpu.make_async_copy(span, span, sem).wait()


def body(n_patch, n_sub, *args):
    nodes, edges, ced, wei, weo, wni, wno, fs, fr, hl, cs, cr = args
    fs, fr, cs, cr = (x.reshape(1, -1) for x in (fs, fr, cs, cr))
    operands = (nodes, edges, ced, wei, weo, wni, wno, fs, fr, hl, cs, cr)
    group = n_patch * n_sub
    n, d = nodes.shape
    e, c = edges.shape[0], ced.shape[0]
    halo = hl.shape[2]
    anywhere = pl.BlockSpec(memory_space=pl.ANY)
    inside = pl.BlockSpec(memory_space=pltpu.VMEM)
    dma = pltpu.SemaphoreType.DMA
    kept = [
        pltpu.VMEM((n, d), BF16),
        pltpu.VMEM((e, d), BF16),
        pltpu.VMEM((c, d), BF16),
        pltpu.VMEM((n, d), BF16),
        pltpu.VMEM((FIRST, d), F32),
        pltpu.VMEM((FIRST, d), F32),
        pltpu.VMEM(wni.shape, BF16),
        pltpu.VMEM(wno.shape, BF16),
    ]
    scratch = [pltpu.VMEM(x.shape, x.dtype) for x in (edges, ced, wei, weo, fs, fr, hl, cs, cr)] + [
        pltpu.VMEM((c, d), BF16),
        pltpu.VMEM((c, d), BF16),
        pltpu.VMEM((2,) + cs.shape, cs.dtype),
        pltpu.VMEM((group, CO_DEV, d), BF16),
        pltpu.VMEM((group * CO_DEV, d), F32),
        pltpu.VMEM((2, halo, d), BF16),
        pltpu.VMEM((2, halo, d), BF16),
        pltpu.VMEM((group * CO_DEV, d), F32),
        pltpu.VMEM((group, CO_DEV, d), BF16),
        pltpu.VMEM((group - n_sub, CO_DEV, d), BF16),
        pltpu.VMEM((e, d), F32),
        pltpu.VMEM((2 * c, d), F32),
        dma((3,)), dma, dma, dma, dma, dma, dma, dma, dma, pltpu.SemaphoreType.REGULAR,
    ]
    held = pl.pallas_call(
        functools.partial(kernel, n_patch, n_sub),
        out_shape=kept,
        in_specs=[anywhere] * len(operands),
        out_specs=[inside] * len(kept),
        scratch_shapes=scratch,
        compiler_params=pltpu.CompilerParams(
            collective_id=0, has_side_effects=True, vmem_limit_bytes=60 * 1024 * 1024),
        name="layer",
    )(*operands)
    return pl.pallas_call(
        finish,
        out_shape=[jax.ShapeDtypeStruct(x.shape, BF16) for x in (nodes, edges, ced)],
        in_specs=[inside] * len(kept),
        out_specs=[anywhere] * 3,
        scratch_shapes=[pltpu.VMEM((FIRST, d), BF16), dma],
        compiler_params=pltpu.CompilerParams(vmem_limit_bytes=8 * 1024 * 1024),
        name="finish",
    )(*held)


def solution(mesh):
    rows = P(("parts", "patch", "sub"), None)
    ids = P(("parts", "patch", "sub"))
    in_specs = (rows, rows, rows, P(), P(), P(), P(), ids, ids,
                P(("parts", "patch", "sub"), None, None), ids, ids)
    run = functools.partial(body, mesh.shape["patch"], mesh.shape["sub"])
    return jax.shard_map(run, mesh=mesh, in_specs=in_specs, out_specs=(rows, rows, rows),
                         check_vma=False)
```

```python
import functools

import jax
import jax.numpy as jnp
from jax import lax
from jax.experimental import pallas as pl
from jax.experimental.pallas import tpu as pltpu
from jax.sharding import PartitionSpec as P

CO_DEV = 4
FIRST = 16
F32 = jnp.float32
BF16 = jnp.bfloat16
MESH = pl.DeviceIdType.MESH


def dot(a, b, dims=((1,), (0,))):
    return lax.dot_general(a, b, (dims, ((), ())), preferred_element_type=F32)


def silu(v):
    half = 0.5 * v
    return (half + half * jnp.tanh(half)).astype(BF16)


def centre(w):
    n = w.shape[1]
    mean = dot(w, jnp.full((n, 128), 1.0, BF16)) * (1.0 / n)
    return jnp.concatenate(
        [(w[:, i:i + 128].astype(F32) - mean).astype(BF16) for i in range(0, n, 128)], axis=1)


def norm_rows(centred):
    return centred * lax.rsqrt(jnp.mean(centred * centred, axis=-1, keepdims=True) + 1e-05)


def column(row):
    n = row.shape[1]
    wide = jnp.broadcast_to(row.astype(F32), (8, n))
    return jnp.transpose(wide)[:, :1]


def hot(col, first, count):
    lanes = lax.broadcasted_iota(jnp.int32, (col.shape[0], count), 1) + first
    return (col == lanes.astype(F32)).astype(BF16)


def hot_t(row, count):
    rows = lax.broadcasted_iota(jnp.int32, (count, row.shape[1]), 0)
    return (rows == row).astype(BF16)


def each(count, step):
    if count <= 16:
        for i in range(count):
            step(i)
    else:
        def run(i, carry):
            step(i)
            return carry

        lax.fori_loop(0, count, run, 0)


def node_rows(rows, pre, w_out):
    return (rows.astype(F32) + norm_rows(dot(silu(pre), w_out))).astype(BF16)


def kernel(
    n_patch, n_sub,
    nodes_h, edges_h, ced_h, wei_h, weo_h, wni_h, wno_h, fs_h, fr_h, hl_h, cs_h, cr_h,
    n_rows, ne_v, nc_v, nodes_v, n_pre, top, wni_v, wno_v,
    edges_v, ced_v, wei_v, weo_v, fs_v, fr_v, hl_v, cs_v, cr_v,
    mate_v, mate_new, mate_ids,
    heads_r, heads_f, halo_s, halo_r, part_f, part_s, part_r,
    acc, ced_pre, weo_raw, wno_raw, in_sem, sent, ag_s, ag_r, halo_rs, rs_s, rs_r, ids_r, mate_r, near,
):
    group, shift = n_patch * n_sub, n_sub
    hub_p = n_patch - 1
    hubs = group - shift
    mp, ms = lax.axis_index("patch"), lax.axis_index("sub")
    me = mp * n_sub + ms
    hub, leaf, hosts = mp < hub_p, mp == hub_p, mp == hub_p - 1
    nodes_n, d = nodes_v.shape
    halo = halo_s.shape[1]
    co = heads_r.shape[1]
    count = ced_v.shape[0]

    def rows_of(i):
        start = i * 2 * co
        return pl.ds(start if isinstance(i, int) else pl.multiple_of(start, 2 * co), 2 * co)

    def turn(i, by, n):
        at = i + by
        return jnp.where(at >= n, at - n, at)

    def device(p, s):
        return {"device_id": {"patch": p, "sub": s}, "device_id_type": MESH}

    def device_of(i):
        if isinstance(i, int):
            return device(i // n_sub, i % n_sub)
        return device(lax.div(i, n_sub), lax.rem(i, n_sub))

    subs = [turn(ms, j, n_sub) for j in list(range(n_sub // 2, n_sub)) + list(range(1, n_sub // 2))]

    def patch(p, step):
        for s in subs + [ms]:
            step(p, s)

    def beside(step):
        for s in subs:
            step(mp, s)

    def await_rows(number, sem):
        span = heads_r.at[pl.ds(0, number)]
        pltpu.make_async_copy(span, span, sem).wait()

    barrier = pltpu.get_barrier_semaphore()

    def hail(p, s):
        pl.semaphore_signal(barrier, inc=1, **device(p, s))

    host, guest = device(mp - 1, ms), device(mp + 1, ms)
    visit = [
        pltpu.make_async_remote_copy(
            src_ref=src, dst_ref=dst, send_sem=out, recv_sem=sem, **host)
        for src, dst, out, sem in (
            (ced_h, mate_v, sent, mate_r),
            (cs_h, mate_ids.at[0], ids_r, ids_r), (cr_h, mate_ids.at[1], ids_r, ids_r))
    ]
    await_ids = pltpu.make_async_copy(mate_ids, mate_ids, ids_r).wait
    back = pltpu.make_async_remote_copy(
        src_ref=mate_new, dst_ref=mate_v, send_sem=sent, recv_sem=mate_r, **guest)

    @pl.when(hub)
    def _():
        patch(turn(mp, 1, hub_p), hail)
        pl.when(hosts)(lambda: hail(mp + 1, ms))
        each(hub_p - 2, lambda i: patch(turn(mp, i + 2, hub_p), hail))
        beside(hail)

    @pl.when(leaf)
    def _():
        pl.semaphore_wait(barrier, 1)
        for copy in visit:
            copy.start()

    groups = [
        [(nodes_h, nodes_v), (hl_h, hl_v)],
        [(fs_h, fs_v), (fr_h, fr_v), (cs_h, cs_v), (cr_h, cr_v), (wei_h, wei_v)],
        [(edges_h, edges_v), (ced_h, ced_v), (weo_h, weo_raw), (wni_h, wni_v), (wno_h, wno_raw)],
    ]
    loads = [[pltpu.make_async_copy(h, v, in_sem.at[i]) for h, v in pairs]
             for i, pairs in enumerate(groups)]
    for copies in loads:
        for copy in copies:
            copy.start()

    def loaded(i):
        for copy in loads[i]:
            copy.wait()

    loaded(0)
    nodes = nodes_v[...]
    head_row = heads_r.at[me]

    def send_head(p, s):
        pltpu.make_async_remote_copy(
            src_ref=head_row, dst_ref=head_row, send_sem=ag_s, recv_sem=ag_r,
            **device(p, s)).start()

    heads_r[me] = nodes[:co]

    @pl.when(hub)
    def _():
        pl.semaphore_wait(barrier, hubs - 1)

        @pl.when(hosts & (lax.rem(ms, 2) == 0))
        def _():
            hail(mp + 1, ms)
            hail(mp + 1, ms + 1)

        each(hub_p - 1, lambda i: patch(turn(mp, hub_p - 1 - i, hub_p), send_head))
        beside(send_head)

    prev, after = turn(me, group - 1, group), turn(me, 1, group)

    def away(i):
        return jnp.where(i >= hubs, 1, 0)

    @pl.when(leaf)
    def _():
        pl.semaphore_wait(barrier, 1)
        each(hub_p, lambda i: patch(hub_p - 1 - i, send_head))
        pl.semaphore_signal(near, inc=1, **host)
        for i in (prev, after):
            pl.semaphore_signal(near, inc=1, **device_of(i - shift * away(i)))

    for side in range(2):
        pick = hot_t(hl_v[0, side:side + 1, :], nodes_n)
        halo_s[side] = dot(pick, nodes, ((0,), (0,))).astype(BF16)

    halos, soon = [], []
    for side, to in ((0, after), (1, prev)):
        soon.append(to < hubs)
        halos.append(pltpu.make_async_remote_copy(
            src_ref=halo_s.at[side], dst_ref=halo_r.at[side],
            send_sem=sent, recv_sem=halo_rs, **device_of(to)))
        pl.when(soon[-1])(halos[-1].start)

    loaded(1)
    fs, fr = fs_v[...], fr_v[...]
    fs_col = column(jnp.where(fs < halo, fs + (nodes_n + halo), fs - halo))
    fr_col = column(fr)
    own = jnp.concatenate(
        [dot(nodes, wei_v[d:2 * d]).astype(BF16), dot(nodes, wei_v[2 * d:]).astype(BF16)], axis=0)
    sel = jnp.concatenate([hot(fs_col, 0, nodes_n), hot(fr_col, 0, nodes_n)], axis=1)
    loaded(2)
    acc[...] = dot(edges_v[...], wei_v[:d]) + dot(sel, own)
    weo_v[...] = centre(weo_raw[...])
    wno_v[...] = centre(wno_raw[...])

    callers = away(prev) + away(after) + jnp.where(
        hosts, 1 + away(me + shift - 1) + away(turn(me + shift, 1, group)), 0)
    pl.when(hub & (callers > 0))(lambda: pl.semaphore_wait(near, callers))
    pl.when(hosts)(lambda: pl.semaphore_signal(near, inc=1, **guest))
    pl.when(leaf)(lambda: pl.semaphore_wait(near, 1))
    for early, copy in zip(soon, halos):
        pl.when(jnp.logical_not(early))(copy.start)

    def coarse(hosting):
        ced, cs, cr = ced_v[...], cs_v[...], cr_v[...]
        ced_pre[:count] = dot(ced, wei_v[:d])
        if hosting:
            await_ids()
            cs = jnp.concatenate([cs, mate_ids[0]], axis=1)
            cr = jnp.concatenate([cr, mate_ids[1]], axis=1)
        rows = cs.shape[1]
        picks = hot_t(cr, group * co)
        ends = jnp.concatenate(
            [hot(column(cs), 0, group * co), hot(column(cr), 0, group * co)], axis=0)
        if hosting:
            visit[0].wait_recv()
            ced_pre[count:] = dot(mate_v[...], wei_v[:d])
            ced = jnp.concatenate([ced, mate_v[...]], axis=0)

        await_rows(group - 1, ag_r)

        def flat(i):
            both = jnp.concatenate(
                [heads_r[2 * i].astype(F32), heads_r[2 * i + 1].astype(F32)], axis=0)
            heads_f[rows_of(i), :] = both

        each(group // 2, flat)
        heads = heads_f[...].astype(BF16)
        c_ends = dot(ends, heads).astype(BF16)
        c_in = jnp.concatenate([c_ends[:rows], c_ends[rows:]], axis=1)
        c_hid = silu(ced_pre[:rows] + dot(c_in, wei_v[d:]))
        c_new = (ced.astype(F32) + norm_rows(dot(c_hid, weo_v[...]))).astype(BF16)
        part_f[...] = dot(picks, c_new)

        def send_part(i):
            pltpu.make_async_remote_copy(
                src_ref=part_s.at[i], dst_ref=part_r.at[me],
                send_sem=rs_s, recv_sem=rs_r, **device_of(i)).start()

        def pack(i):
            both = part_f[rows_of(i), :].astype(BF16)
            for j in range(2):
                at = 2 * i + j
                part_s[at] = both[j * co:(j + 1) * co]
                pl.when(me != at)(lambda: send_part(at))

        each(group // 2, pack)
        if hosting:
            mate_new[...] = c_new[count:]
            back.start()
        part_r[me] = part_s[me]
        nc_v[...] = c_new[:count]

    pl.when(hub & jnp.logical_not(hosts))(lambda: coarse(False))
    pl.when(hosts)(lambda: coarse(True))

    pltpu.make_async_copy(halo_r, halo_r, halo_rs).wait()
    far = dot(jnp.concatenate([halo_r[1], halo_r[0]], axis=0), wei_v[d:2 * d]).astype(BF16)
    hid = silu(acc[...] + dot(hot(fs_col, nodes_n, 2 * halo), far))
    delta = norm_rows(dot(hid, weo_v[...]))
    e_new = (edges_v[...].astype(F32) + jnp.where(fr_col >= 0.0, delta, 0.0)).astype(BF16)
    ne_v[...] = e_new
    fine = dot(hot_t(fr, nodes_n), e_new)

    pre = dot(nodes, wni_v[:d])
    n_rows[...] = node_rows(nodes, pre + dot(fine.astype(BF16), wni_v[d:]), wno_v[...])
    first = top.shape[0]
    n_pre[...] = pre[:first]
    top[...] = fine[:first]

    def await_sent(rows):
        span = edges_v.at[pl.ds(0, rows)]
        pltpu.make_async_copy(span, span, sent).wait()

    pl.when(mp < hub_p - 1)(lambda: await_sent(2 * halo))
    pl.when(mp >= hub_p - 1)(lambda: await_sent(2 * halo + count))

    @pl.when(hub)
    def _():
        await_rows(hubs - 1, ag_s)
        await_rows(group - 1, rs_s)
        await_rows(hubs - 1, rs_r)

    @pl.when(leaf)
    def _():
        await_rows(hubs, ag_s)
        await_ids()
        back.wait_recv()
        nc_v[...] = mate_v[...]
        await_rows(hubs, rs_r)

    top[:co] += jnp.sum(part_r[...].astype(F32), axis=0)


def finish(n_rows, ne_v, nc_v, nodes_v, n_pre, top, wni_v, wno_v, nn_h, ne_h, nc_h, first_v, sem):
    first, d = top.shape
    n = n_rows.shape[0]
    for src, dst in (
            (ne_v, ne_h), (nc_v, nc_h),
            (n_rows.at[pl.ds(first, n - first)], nn_h.at[pl.ds(first, n - first)])):
        pltpu.make_async_copy(src, dst, sem).start()
    pre = n_pre[...] + dot(top[...].astype(BF16), wni_v[d:])
    first_v[...] = node_rows(nodes_v[:first], pre, wno_v[...])
    pltpu.make_async_copy(first_v, nn_h.at[pl.ds(0, first)], sem).start()
    span = wni_v.at[pl.ds(0, ne_v.shape[0] + nc_v.shape[0] + n)]
    pltpu.make_async_copy(span, span, sem).wait()


def body(n_patch, n_sub, *args):
    nodes, edges, ced, wei, weo, wni, wno, fs, fr, hl, cs, cr = args
    fs, fr, cs, cr = (x.reshape(1, -1) for x in (fs, fr, cs, cr))
    operands = (nodes, edges, ced, wei, weo, wni, wno, fs, fr, hl, cs, cr)
    group = n_patch * n_sub
    n, d = nodes.shape
    e, c = edges.shape[0], ced.shape[0]
    halo = hl.shape[2]
    anywhere = pl.BlockSpec(memory_space=pl.ANY)
    inside = pl.BlockSpec(memory_space=pltpu.VMEM)
    dma = pltpu.SemaphoreType.DMA
    kept = [
        pltpu.VMEM((n, d), BF16),
        pltpu.VMEM((e, d), BF16),
        pltpu.VMEM((c, d), BF16),
        pltpu.VMEM((n, d), BF16),
        pltpu.VMEM((FIRST, d), F32),
        pltpu.VMEM((FIRST, d), F32),
        pltpu.VMEM(wni.shape, BF16),
        pltpu.VMEM(wno.shape, BF16),
    ]
    scratch = [pltpu.VMEM(x.shape, x.dtype) for x in (edges, ced, wei, weo, fs, fr, hl, cs, cr)] + [
        pltpu.VMEM((c, d), BF16),
        pltpu.VMEM((c, d), BF16),
        pltpu.VMEM((2,) + cs.shape, cs.dtype),
        pltpu.VMEM((group, CO_DEV, d), BF16),
        pltpu.VMEM((group * CO_DEV, d), F32),
        pltpu.VMEM((2, halo, d), BF16),
        pltpu.VMEM((2, halo, d), BF16),
        pltpu.VMEM((group * CO_DEV, d), F32),
        pltpu.VMEM((group, CO_DEV, d), BF16),
        pltpu.VMEM((group - n_sub, CO_DEV, d), BF16),
        pltpu.VMEM((e, d), F32),
        pltpu.VMEM((2 * c, d), F32),
        pltpu.VMEM(weo.shape, BF16),
        pltpu.VMEM(wno.shape, BF16),
        dma((3,)), dma, dma, dma, dma, dma, dma, dma, dma, pltpu.SemaphoreType.REGULAR,
    ]
    held = pl.pallas_call(
        functools.partial(kernel, n_patch, n_sub),
        out_shape=kept,
        in_specs=[anywhere] * len(operands),
        out_specs=[inside] * len(kept),
        scratch_shapes=scratch,
        compiler_params=pltpu.CompilerParams(
            collective_id=0, has_side_effects=True, vmem_limit_bytes=60 * 1024 * 1024),
        name="layer",
    )(*operands)
    return pl.pallas_call(
        finish,
        out_shape=[jax.ShapeDtypeStruct(x.shape, BF16) for x in (nodes, edges, ced)],
        in_specs=[inside] * len(kept),
        out_specs=[anywhere] * 3,
        scratch_shapes=[pltpu.VMEM((FIRST, d), BF16), dma],
        compiler_params=pltpu.CompilerParams(vmem_limit_bytes=8 * 1024 * 1024),
        name="finish",
    )(*held)


def solution(mesh):
    rows = P(("parts", "patch", "sub"), None)
    ids = P(("parts", "patch", "sub"))
    in_specs = (rows, rows, rows, P(), P(), P(), P(), ids, ids,
                P(("parts", "patch", "sub"), None, None), ids, ids)
    run = functools.partial(body, mesh.shape["patch"], mesh.shape["sub"])
    return jax.shard_map(run, mesh=mesh, in_specs=in_specs, out_specs=(rows, rows, rows),
                         check_vma=False)
```

```python
import functools

import jax
import jax.numpy as jnp
from jax import lax
from jax.experimental import pallas as pl
from jax.experimental.pallas import tpu as pltpu
from jax.sharding import PartitionSpec as P

CO_DEV = 4
FIRST = 16
F32 = jnp.float32
BF16 = jnp.bfloat16
MESH = pl.DeviceIdType.MESH


def dot(a, b, dims=((1,), (0,))):
    return lax.dot_general(a, b, (dims, ((), ())), preferred_element_type=F32)


def silu(v):
    half = 0.5 * v
    return (half + half * jnp.tanh(half)).astype(BF16)


def centre(w):
    n = w.shape[1]
    mean = dot(w, jnp.full((n, 128), 1.0, BF16)) * (1.0 / n)
    return jnp.concatenate(
        [(w[:, i:i + 128].astype(F32) - mean).astype(BF16) for i in range(0, n, 128)], axis=1)


def norm_rows(centred):
    return centred * lax.rsqrt(jnp.mean(centred * centred, axis=-1, keepdims=True) + 1e-05)


def column(row):
    n = row.shape[1]
    wide = jnp.broadcast_to(row.astype(F32), (8, n))
    return jnp.transpose(wide)[:, :1]


def hot(col, first, count):
    lanes = lax.broadcasted_iota(jnp.int32, (col.shape[0], count), 1) + first
    return (col == lanes.astype(F32)).astype(BF16)


def hot_t(row, count):
    rows = lax.broadcasted_iota(jnp.int32, (count, row.shape[1]), 0)
    return (rows == row).astype(BF16)


def each(count, step):
    if count <= 16:
        for i in range(count):
            step(i)
    else:
        def run(i, carry):
            step(i)
            return carry

        lax.fori_loop(0, count, run, 0)


def node_rows(rows, pre, w_out):
    return (rows.astype(F32) + norm_rows(dot(silu(pre), w_out))).astype(BF16)


def kernel(
    n_patch, n_sub,
    nodes_h, edges_h, ced_h, wei_h, weo_h, wni_h, wno_h, fs_h, fr_h, hl_h, cs_h, cr_h,
    n_rows, ne_v, nc_v, nodes_v, n_pre, top, wni_v, wno_v,
    edges_v, ced_v, wei_v, weo_v, fs_v, fr_v, hl_v, cs_v, cr_v,
    mate_v, mate_new, mate_ids,
    heads_r, heads_f, halo_s, halo_r, part_f, part_s, part_r,
    acc, ced_pre, weo_raw, wno_raw, in_sem, sent, ag_s, ag_r, halo_rs, rs_s, rs_r, ids_r, mate_r, near,
):
    group, shift = n_patch * n_sub, n_sub
    hub_p = n_patch - 1
    hubs = group - shift
    mp, ms = lax.axis_index("patch"), lax.axis_index("sub")
    me = mp * n_sub + ms
    hub, leaf, hosts = mp < hub_p, mp == hub_p, mp == hub_p - 1
    nodes_n, d = nodes_v.shape
    halo = halo_s.shape[1]
    co = heads_r.shape[1]
    count = ced_v.shape[0]

    def rows_of(i):
        start = i * 2 * co
        return pl.ds(start if isinstance(i, int) else pl.multiple_of(start, 2 * co), 2 * co)

    def turn(i, by, n):
        at = i + by
        return jnp.where(at >= n, at - n, at)

    def device(p, s):
        return {"device_id": {"patch": p, "sub": s}, "device_id_type": MESH}

    def device_of(i):
        if isinstance(i, int):
            return device(i // n_sub, i % n_sub)
        return device(lax.div(i, n_sub), lax.rem(i, n_sub))

    subs = [turn(ms, j, n_sub) for j in list(range(n_sub // 2, n_sub)) + list(range(1, n_sub // 2))]

    def patch(p, step):
        for s in subs + [ms]:
            step(p, s)

    def beside(step):
        for s in subs:
            step(mp, s)

    def await_rows(number, sem):
        span = heads_r.at[pl.ds(0, number)]
        pltpu.make_async_copy(span, span, sem).wait()

    barrier = pltpu.get_barrier_semaphore()

    def hail(p, s):
        pl.semaphore_signal(barrier, inc=1, **device(p, s))

    host, guest = device(mp - 1, ms), device(mp + 1, ms)
    visit = [
        pltpu.make_async_remote_copy(
            src_ref=src, dst_ref=dst, send_sem=out, recv_sem=sem, **host)
        for src, dst, out, sem in (
            (ced_h, mate_v, sent, mate_r),
            (cs_h, mate_ids.at[0], ids_r, ids_r), (cr_h, mate_ids.at[1], ids_r, ids_r))
    ]
    await_ids = pltpu.make_async_copy(mate_ids, mate_ids, ids_r).wait
    back = pltpu.make_async_remote_copy(
        src_ref=mate_new, dst_ref=mate_v, send_sem=sent, recv_sem=mate_r, **guest)

    @pl.when(hub)
    def _():
        patch(turn(mp, 1, hub_p), hail)
        pl.when(hosts)(lambda: hail(mp + 1, ms))
        each(hub_p - 2, lambda i: patch(turn(mp, i + 2, hub_p), hail))
        beside(hail)

    @pl.when(leaf)
    def _():
        pl.semaphore_wait(barrier, 1)
        for copy in visit:
            copy.start()

    groups = [
        [(nodes_h, nodes_v), (hl_h, hl_v)],
        [(fs_h, fs_v), (fr_h, fr_v), (cs_h, cs_v), (cr_h, cr_v), (wei_h, wei_v)],
        [(edges_h, edges_v), (ced_h, ced_v), (weo_h, weo_raw), (wni_h, wni_v), (wno_h, wno_raw)],
    ]
    loads = [[pltpu.make_async_copy(h, v, in_sem.at[i]) for h, v in pairs]
             for i, pairs in enumerate(groups)]
    for copies in loads:
        for copy in copies:
            copy.start()

    def loaded(i):
        for copy in loads[i]:
            copy.wait()

    loaded(0)
    nodes = nodes_v[...]
    head_row = heads_r.at[me]

    def send_head(p, s):
        pltpu.make_async_remote_copy(
            src_ref=head_row, dst_ref=head_row, send_sem=ag_s, recv_sem=ag_r,
            **device(p, s)).start()

    heads_r[me] = nodes[:co]

    @pl.when(hub)
    def _():
        pl.semaphore_wait(barrier, hubs - 1)
        pl.when(hosts)(lambda: hail(mp + 1, ms))
        each(hub_p - 1, lambda i: patch(turn(mp, hub_p - 1 - i, hub_p), send_head))
        beside(send_head)

    prev, after = turn(me, group - 1, group), turn(me, 1, group)

    def away(i):
        return jnp.where(i >= hubs, 1, 0)

    @pl.when(leaf)
    def _():
        pl.semaphore_wait(barrier, 1)
        each(hub_p, lambda i: patch(hub_p - 1 - i, send_head))
        pl.semaphore_signal(near, inc=1, **host)
        for i in (prev, after):
            pl.semaphore_signal(near, inc=1, **device_of(i - shift * away(i)))

    for side in range(2):
        pick = hot_t(hl_v[0, side:side + 1, :], nodes_n)
        halo_s[side] = dot(pick, nodes, ((0,), (0,))).astype(BF16)

    halos, soon = [], []
    for side, to in ((0, after), (1, prev)):
        soon.append(to < hubs)
        halos.append(pltpu.make_async_remote_copy(
            src_ref=halo_s.at[side], dst_ref=halo_r.at[side],
            send_sem=sent, recv_sem=halo_rs, **device_of(to)))
        pl.when(soon[-1])(halos[-1].start)

    loaded(1)
    fs, fr = fs_v[...], fr_v[...]
    fs_col = column(jnp.where(fs < halo, fs + (nodes_n + halo), fs - halo))
    fr_col = column(fr)
    own = jnp.concatenate(
        [dot(nodes, wei_v[d:2 * d]).astype(BF16), dot(nodes, wei_v[2 * d:]).astype(BF16)], axis=0)
    sel = jnp.concatenate([hot(fs_col, 0, nodes_n), hot(fr_col, 0, nodes_n)], axis=1)
    loaded(2)
    acc[...] = dot(edges_v[...], wei_v[:d]) + dot(sel, own)
    weo_v[...] = centre(weo_raw[...])
    wno_v[...] = centre(wno_raw[...])

    callers = away(prev) + away(after) + jnp.where(
        hosts, 1 + away(me + shift - 1) + away(turn(me + shift, 1, group)), 0)
    pl.when(hub & (callers > 0))(lambda: pl.semaphore_wait(near, callers))
    pl.when(hosts)(lambda: pl.semaphore_signal(near, inc=1, **guest))
    pl.when(leaf)(lambda: pl.semaphore_wait(near, 1))
    for early, copy in zip(soon, halos):
        pl.when(jnp.logical_not(early))(copy.start)

    def coarse(hosting):
        ced, cs, cr = ced_v[...], cs_v[...], cr_v[...]
        ced_pre[:count] = dot(ced, wei_v[:d])
        if hosting:
            await_ids()
            cs = jnp.concatenate([cs, mate_ids[0]], axis=1)
            cr = jnp.concatenate([cr, mate_ids[1]], axis=1)
        rows = cs.shape[1]
        picks = hot_t(cr, group * co)
        ends = jnp.concatenate(
            [hot(column(cs), 0, group * co), hot(column(cr), 0, group * co)], axis=0)
        if hosting:
            visit[0].wait_recv()
            ced_pre[count:] = dot(mate_v[...], wei_v[:d])
            ced = jnp.concatenate([ced, mate_v[...]], axis=0)

        await_rows(group - 1, ag_r)

        def flat(i):
            both = jnp.concatenate(
                [heads_r[2 * i].astype(F32), heads_r[2 * i + 1].astype(F32)], axis=0)
            heads_f[rows_of(i), :] = both

        each(group // 2, flat)
        heads = heads_f[...].astype(BF16)
        c_ends = dot(ends, heads).astype(BF16)
        c_in = jnp.concatenate([c_ends[:rows], c_ends[rows:]], axis=1)
        c_hid = silu(ced_pre[:rows] + dot(c_in, wei_v[d:]))
        c_new = (ced.astype(F32) + norm_rows(dot(c_hid, weo_v[...]))).astype(BF16)
        part_f[...] = dot(picks, c_new)

        def send_part(i):
            pltpu.make_async_remote_copy(
                src_ref=part_s.at[i], dst_ref=part_r.at[me],
                send_sem=rs_s, recv_sem=rs_r, **device_of(i)).start()

        def pack(i):
            both = part_f[rows_of(i), :].astype(BF16)
            for j in range(2):
                at = 2 * i + j
                part_s[at] = both[j * co:(j + 1) * co]
                pl.when(me != at)(lambda: send_part(at))

        each(group // 2, pack)
        if hosting:
            mate_new[...] = c_new[count:]
            back.start()
        part_r[me] = part_s[me]
        nc_v[...] = c_new[:count]

    pl.when(hub & jnp.logical_not(hosts))(lambda: coarse(False))
    pl.when(hosts)(lambda: coarse(True))

    pltpu.make_async_copy(halo_r, halo_r, halo_rs).wait()
    far = dot(jnp.concatenate([halo_r[1], halo_r[0]], axis=0), wei_v[d:2 * d]).astype(BF16)
    hid = silu(acc[...] + dot(hot(fs_col, nodes_n, 2 * halo), far))
    delta = norm_rows(dot(hid, weo_v[...]))
    e_new = (edges_v[...].astype(F32) + jnp.where(fr_col >= 0.0, delta, 0.0)).astype(BF16)
    ne_v[...] = e_new
    fine = dot(hot_t(fr, nodes_n), e_new)

    pre = dot(nodes, wni_v[:d])
    n_rows[...] = node_rows(nodes, pre + dot(fine.astype(BF16), wni_v[d:]), wno_v[...])
    first = top.shape[0]
    n_pre[...] = pre[:first]
    top[...] = fine[:first]

    def await_sent(rows):
        span = edges_v.at[pl.ds(0, rows)]
        pltpu.make_async_copy(span, span, sent).wait()

    pl.when(mp < hub_p - 1)(lambda: await_sent(2 * halo))
    pl.when(mp >= hub_p - 1)(lambda: await_sent(2 * halo + count))

    @pl.when(hub)
    def _():
        await_rows(hubs - 1, ag_s)
        await_rows(group - 1, rs_s)
        await_rows(hubs - 1, rs_r)

    @pl.when(leaf)
    def _():
        await_rows(hubs, ag_s)
        await_ids()
        back.wait_recv()
        nc_v[...] = mate_v[...]
        await_rows(hubs, rs_r)

    top[:co] += jnp.sum(part_r[...].astype(F32), axis=0)


def finish(n_rows, ne_v, nc_v, nodes_v, n_pre, top, wni_v, wno_v, nn_h, ne_h, nc_h, first_v, sem):
    first, d = top.shape
    n = n_rows.shape[0]
    for src, dst in (
            (ne_v, ne_h), (nc_v, nc_h),
            (n_rows.at[pl.ds(first, n - first)], nn_h.at[pl.ds(first, n - first)])):
        pltpu.make_async_copy(src, dst, sem).start()
    pre = n_pre[...] + dot(top[...].astype(BF16), wni_v[d:])
    first_v[...] = node_rows(nodes_v[:first], pre, wno_v[...])
    pltpu.make_async_copy(first_v, nn_h.at[pl.ds(0, first)], sem).start()
    span = wni_v.at[pl.ds(0, ne_v.shape[0] + nc_v.shape[0] + n)]
    pltpu.make_async_copy(span, span, sem).wait()


def body(n_patch, n_sub, *args):
    nodes, edges, ced, wei, weo, wni, wno, fs, fr, hl, cs, cr = args
    fs, fr, cs, cr = (x.reshape(1, -1) for x in (fs, fr, cs, cr))
    operands = (nodes, edges, ced, wei, weo, wni, wno, fs, fr, hl, cs, cr)
    group = n_patch * n_sub
    n, d = nodes.shape
    e, c = edges.shape[0], ced.shape[0]
    halo = hl.shape[2]
    anywhere = pl.BlockSpec(memory_space=pl.ANY)
    inside = pl.BlockSpec(memory_space=pltpu.VMEM)
    dma = pltpu.SemaphoreType.DMA
    kept = [
        pltpu.VMEM((n, d), BF16),
        pltpu.VMEM((e, d), BF16),
        pltpu.VMEM((c, d), BF16),
        pltpu.VMEM((n, d), BF16),
        pltpu.VMEM((FIRST, d), F32),
        pltpu.VMEM((FIRST, d), F32),
        pltpu.VMEM(wni.shape, BF16),
        pltpu.VMEM(wno.shape, BF16),
    ]
    scratch = [pltpu.VMEM(x.shape, x.dtype) for x in (edges, ced, wei, weo, fs, fr, hl, cs, cr)] + [
        pltpu.VMEM((c, d), BF16),
        pltpu.VMEM((c, d), BF16),
        pltpu.VMEM((2,) + cs.shape, cs.dtype),
        pltpu.VMEM((group, CO_DEV, d), BF16),
        pltpu.VMEM((group * CO_DEV, d), F32),
        pltpu.VMEM((2, halo, d), BF16),
        pltpu.VMEM((2, halo, d), BF16),
        pltpu.VMEM((group * CO_DEV, d), F32),
        pltpu.VMEM((group, CO_DEV, d), BF16),
        pltpu.VMEM((group - n_sub, CO_DEV, d), BF16),
        pltpu.VMEM((e, d), F32),
        pltpu.VMEM((2 * c, d), F32),
        pltpu.VMEM(weo.shape, BF16),
        pltpu.VMEM(wno.shape, BF16),
        dma((3,)), dma, dma, dma, dma, dma, dma, dma, dma, pltpu.SemaphoreType.REGULAR,
    ]
    held = pl.pallas_call(
        functools.partial(kernel, n_patch, n_sub),
        out_shape=kept,
        in_specs=[anywhere] * len(operands),
        out_specs=[inside] * len(kept),
        scratch_shapes=scratch,
        compiler_params=pltpu.CompilerParams(
            collective_id=0, has_side_effects=True, vmem_limit_bytes=60 * 1024 * 1024),
        name="layer",
    )(*operands)
    return pl.pallas_call(
        finish,
        out_shape=[jax.ShapeDtypeStruct(x.shape, BF16) for x in (nodes, edges, ced)],
        in_specs=[inside] * len(kept),
        out_specs=[anywhere] * 3,
        scratch_shapes=[pltpu.VMEM((FIRST, d), BF16), dma],
        compiler_params=pltpu.CompilerParams(vmem_limit_bytes=8 * 1024 * 1024),
        name="finish",
    )(*held)


def solution(mesh):
    rows = P(("parts", "patch", "sub"), None)
    ids = P(("parts", "patch", "sub"))
    in_specs = (rows, rows, rows, P(), P(), P(), P(), ids, ids,
                P(("parts", "patch", "sub"), None, None), ids, ids)
    run = functools.partial(body, mesh.shape["patch"], mesh.shape["sub"])
    return jax.shard_map(run, mesh=mesh, in_specs=in_specs, out_specs=(rows, rows, rows),
                         check_vma=False)
```

```python
import functools

import jax
import jax.numpy as jnp
from jax import lax
from jax.experimental import pallas as pl
from jax.experimental.pallas import tpu as pltpu
from jax.sharding import PartitionSpec as P

CO_DEV = 4
FIRST = 8
F32 = jnp.float32
BF16 = jnp.bfloat16
MESH = pl.DeviceIdType.MESH


def dot(a, b, dims=((1,), (0,))):
    return lax.dot_general(a, b, (dims, ((), ())), preferred_element_type=F32)


def silu(v):
    half = 0.5 * v
    return (half + half * jnp.tanh(half)).astype(BF16)


def centre(w):
    n = w.shape[1]
    mean = dot(w, jnp.full((n, 128), 1.0, BF16)) * (1.0 / n)
    return jnp.concatenate(
        [(w[:, i:i + 128].astype(F32) - mean).astype(BF16) for i in range(0, n, 128)], axis=1)


def norm_rows(centred):
    return centred * lax.rsqrt(jnp.mean(centred * centred, axis=-1, keepdims=True) + 1e-05)


def column(row):
    n = row.shape[1]
    wide = jnp.broadcast_to(row.astype(F32), (8, n))
    return jnp.transpose(wide)[:, :1]


def hot(col, first, count):
    lanes = lax.broadcasted_iota(jnp.int32, (col.shape[0], count), 1) + first
    return (col == lanes.astype(F32)).astype(BF16)


def hot_t(row, count):
    rows = lax.broadcasted_iota(jnp.int32, (count, row.shape[1]), 0)
    return (rows == row).astype(BF16)


def each(count, step):
    if count <= 16:
        for i in range(count):
            step(i)
    else:
        def run(i, carry):
            step(i)
            return carry

        lax.fori_loop(0, count, run, 0)


def node_rows(rows, pre, w_out):
    return (rows.astype(F32) + norm_rows(dot(silu(pre), w_out))).astype(BF16)


def kernel(
    n_patch, n_sub,
    nodes_h, edges_h, ced_h, wei_h, weo_h, wni_h, wno_h, fs_h, fr_h, hl_h, cs_h, cr_h,
    n_rows, ne_v, nc_v, nodes_v, n_pre, top, wni_v, wno_v,
    edges_v, ced_v, wei_v, weo_v, fs_v, fr_v, hl_v, cs_v, cr_v,
    mate_v, mate_new, mate_ids,
    heads_r, heads_f, halo_s, halo_r, part_f, part_s, part_r,
    acc, ced_pre, weo_raw, wno_raw, in_sem, sent, ag_s, ag_r, halo_rs, rs_s, rs_r, ids_r, mate_r, near,
):
    group, shift = n_patch * n_sub, n_sub
    hub_p = n_patch - 1
    hubs = group - shift
    mp, ms = lax.axis_index("patch"), lax.axis_index("sub")
    me = mp * n_sub + ms
    hub, leaf, hosts = mp < hub_p, mp == hub_p, mp == hub_p - 1
    nodes_n, d = nodes_v.shape
    halo = halo_s.shape[1]
    co = heads_r.shape[1]
    count = ced_v.shape[0]

    def rows_of(i):
        start = i * 2 * co
        return pl.ds(start if isinstance(i, int) else pl.multiple_of(start, 2 * co), 2 * co)

    def turn(i, by, n):
        at = i + by
        return jnp.where(at >= n, at - n, at)

    def device(p, s):
        return {"device_id": {"patch": p, "sub": s}, "device_id_type": MESH}

    def device_of(i):
        if isinstance(i, int):
            return device(i // n_sub, i % n_sub)
        return device(lax.div(i, n_sub), lax.rem(i, n_sub))

    subs = [turn(ms, j, n_sub) for j in list(range(n_sub // 2, n_sub)) + list(range(1, n_sub // 2))]

    def patch(p, step):
        for s in subs + [ms]:
            step(p, s)

    def beside(step):
        for s in subs:
            step(mp, s)

    def await_rows(number, sem):
        span = heads_r.at[pl.ds(0, number)]
        pltpu.make_async_copy(span, span, sem).wait()

    barrier = pltpu.get_barrier_semaphore()

    def hail(p, s):
        pl.semaphore_signal(barrier, inc=1, **device(p, s))

    host, guest = device(mp - 1, ms), device(mp + 1, ms)
    visit = [
        pltpu.make_async_remote_copy(
            src_ref=src, dst_ref=dst, send_sem=out, recv_sem=sem, **host)
        for src, dst, out, sem in (
            (ced_h, mate_v, sent, mate_r),
            (cs_h, mate_ids.at[0], ids_r, ids_r), (cr_h, mate_ids.at[1], ids_r, ids_r))
    ]
    await_ids = pltpu.make_async_copy(mate_ids, mate_ids, ids_r).wait
    back = pltpu.make_async_remote_copy(
        src_ref=mate_new, dst_ref=mate_v, send_sem=sent, recv_sem=mate_r, **guest)

    @pl.when(hub)
    def _():
        patch(turn(mp, 1, hub_p), hail)
        pl.when(hosts)(lambda: hail(mp + 1, ms))
        each(hub_p - 2, lambda i: patch(turn(mp, i + 2, hub_p), hail))
        beside(hail)

    @pl.when(leaf)
    def _():
        pl.semaphore_wait(barrier, 1)
        for copy in visit:
            copy.start()

    groups = [
        [(nodes_h, nodes_v), (hl_h, hl_v)],
        [(fs_h, fs_v), (fr_h, fr_v), (cs_h, cs_v), (cr_h, cr_v), (wei_h, wei_v)],
        [(edges_h, edges_v), (ced_h, ced_v), (weo_h, weo_raw), (wni_h, wni_v), (wno_h, wno_raw)],
    ]
    loads = [[pltpu.make_async_copy(h, v, in_sem.at[i]) for h, v in pairs]
             for i, pairs in enumerate(groups)]
    for copies in loads:
        for copy in copies:
            copy.start()

    def loaded(i):
        for copy in loads[i]:
            copy.wait()

    loaded(0)
    nodes = nodes_v[...]
    head_row = heads_r.at[me]

    def send_head(p, s):
        pltpu.make_async_remote_copy(
            src_ref=head_row, dst_ref=head_row, send_sem=ag_s, recv_sem=ag_r,
            **device(p, s)).start()

    heads_r[me] = nodes[:co]

    @pl.when(hub)
    def _():
        pl.semaphore_wait(barrier, hubs - 1)
        pl.when(hosts)(lambda: hail(mp + 1, ms))
        each(hub_p - 1, lambda i: patch(turn(mp, hub_p - 1 - i, hub_p), send_head))
        beside(send_head)

    prev, after = turn(me, group - 1, group), turn(me, 1, group)

    def away(i):
        return jnp.where(i >= hubs, 1, 0)

    @pl.when(leaf)
    def _():
        pl.semaphore_wait(barrier, 1)
        each(hub_p, lambda i: patch(hub_p - 1 - i, send_head))
        pl.semaphore_signal(near, inc=1, **host)
        for i in (prev, after):
            pl.semaphore_signal(near, inc=1, **device_of(i - shift * away(i)))

    for side in range(2):
        pick = hot_t(hl_v[0, side:side + 1, :], nodes_n)
        halo_s[side] = dot(pick, nodes, ((0,), (0,))).astype(BF16)

    halos, soon = [], []
    for side, to in ((0, after), (1, prev)):
        soon.append(to < hubs)
        halos.append(pltpu.make_async_remote_copy(
            src_ref=halo_s.at[side], dst_ref=halo_r.at[side],
            send_sem=sent, recv_sem=halo_rs, **device_of(to)))
        pl.when(soon[-1])(halos[-1].start)

    loaded(1)
    fs, fr = fs_v[...], fr_v[...]
    fs_col = column(jnp.where(fs < halo, fs + (nodes_n + halo), fs - halo))
    fr_col = column(fr)
    own = jnp.concatenate(
        [dot(nodes, wei_v[d:2 * d]).astype(BF16), dot(nodes, wei_v[2 * d:]).astype(BF16)], axis=0)
    sel = jnp.concatenate([hot(fs_col, 0, nodes_n), hot(fr_col, 0, nodes_n)], axis=1)
    loaded(2)
    acc[...] = dot(edges_v[...], wei_v[:d]) + dot(sel, own)
    weo_v[...] = centre(weo_raw[...])
    wno_v[...] = centre(wno_raw[...])

    callers = away(prev) + away(after) + jnp.where(
        hosts, 1 + away(me + shift - 1) + away(turn(me + shift, 1, group)), 0)
    pl.when(hub & (callers > 0))(lambda: pl.semaphore_wait(near, callers))
    pl.when(hosts)(lambda: pl.semaphore_signal(near, inc=1, **guest))
    pl.when(leaf)(lambda: pl.semaphore_wait(near, 1))
    for early, copy in zip(soon, halos):
        pl.when(jnp.logical_not(early))(copy.start)

    def coarse(hosting):
        ced, cs, cr = ced_v[...], cs_v[...], cr_v[...]
        ced_pre[:count] = dot(ced, wei_v[:d])
        if hosting:
            await_ids()
            cs = jnp.concatenate([cs, mate_ids[0]], axis=1)
            cr = jnp.concatenate([cr, mate_ids[1]], axis=1)
        rows = cs.shape[1]
        picks = hot_t(cr, group * co)
        ends = jnp.concatenate(
            [hot(column(cs), 0, group * co), hot(column(cr), 0, group * co)], axis=0)
        if hosting:
            visit[0].wait_recv()
            ced_pre[count:] = dot(mate_v[...], wei_v[:d])
            ced = jnp.concatenate([ced, mate_v[...]], axis=0)

        await_rows(group - 1, ag_r)

        def flat(i):
            both = jnp.concatenate(
                [heads_r[2 * i].astype(F32), heads_r[2 * i + 1].astype(F32)], axis=0)
            heads_f[rows_of(i), :] = both

        each(group // 2, flat)
        heads = heads_f[...].astype(BF16)
        c_ends = dot(ends, heads).astype(BF16)
        c_in = jnp.concatenate([c_ends[:rows], c_ends[rows:]], axis=1)
        c_hid = silu(ced_pre[:rows] + dot(c_in, wei_v[d:]))
        c_new = (ced.astype(F32) + norm_rows(dot(c_hid, weo_v[...]))).astype(BF16)
        part_f[...] = dot(picks, c_new)

        if hosting:
            mate_new[...] = c_new[count:]

        def send_part(i):
            pltpu.make_async_remote_copy(
                src_ref=part_s.at[i], dst_ref=part_r.at[me],
                send_sem=rs_s, recv_sem=rs_r, **device_of(i)).start()

        def pack(i):
            both = part_f[rows_of(i), :].astype(BF16)
            part_s[2 * i] = both[:co]
            part_s[2 * i + 1] = both[co:]

        def send(i):
            for at in (2 * i, 2 * i + 1):
                pl.when(me != at)(lambda at=at: send_part(at))

        def pack_ahead(i):
            pack(i + 1)
            send(i)

        pack(0)
        each(group // 2 - 1, pack_ahead)
        send(group // 2 - 1)
        if hosting:
            back.start()
        part_r[me] = part_s[me]
        nc_v[...] = c_new[:count]

    pl.when(hub & jnp.logical_not(hosts))(lambda: coarse(False))
    pl.when(hosts)(lambda: coarse(True))

    pltpu.make_async_copy(halo_r, halo_r, halo_rs).wait()
    far = dot(jnp.concatenate([halo_r[1], halo_r[0]], axis=0), wei_v[d:2 * d]).astype(BF16)
    hid = silu(acc[...] + dot(hot(fs_col, nodes_n, 2 * halo), far))
    delta = norm_rows(dot(hid, weo_v[...]))
    e_new = (edges_v[...].astype(F32) + jnp.where(fr_col >= 0.0, delta, 0.0)).astype(BF16)
    ne_v[...] = e_new
    fine = dot(hot_t(fr, nodes_n), e_new)

    pre = dot(nodes, wni_v[:d])
    n_rows[...] = node_rows(nodes, pre + dot(fine.astype(BF16), wni_v[d:]), wno_v[...])
    first = top.shape[0]
    n_pre[...] = pre[:first]
    top[...] = fine[:first]

    def await_sent(rows):
        span = edges_v.at[pl.ds(0, rows)]
        pltpu.make_async_copy(span, span, sent).wait()

    pl.when(mp < hub_p - 1)(lambda: await_sent(2 * halo))
    pl.when(mp >= hub_p - 1)(lambda: await_sent(2 * halo + count))

    @pl.when(hub)
    def _():
        await_rows(hubs - 1, ag_s)
        await_rows(group - 1, rs_s)
        await_rows(hubs - 1, rs_r)

    @pl.when(leaf)
    def _():
        await_rows(hubs, ag_s)
        await_ids()
        back.wait_recv()
        nc_v[...] = mate_v[...]
        await_rows(hubs, rs_r)

    top[:co] += jnp.sum(part_r[...].astype(F32), axis=0)


def finish(n_rows, ne_v, nc_v, nodes_v, n_pre, top, wni_v, wno_v, nn_h, ne_h, nc_h, first_v, sem):
    first, d = top.shape
    n = n_rows.shape[0]
    for src, dst in (
            (ne_v, ne_h), (nc_v, nc_h),
            (n_rows.at[pl.ds(first, n - first)], nn_h.at[pl.ds(first, n - first)])):
        pltpu.make_async_copy(src, dst, sem).start()
    pre = n_pre[...] + dot(top[...].astype(BF16), wni_v[d:])
    first_v[...] = node_rows(nodes_v[:first], pre, wno_v[...])
    pltpu.make_async_copy(first_v, nn_h.at[pl.ds(0, first)], sem).start()
    span = wni_v.at[pl.ds(0, ne_v.shape[0] + nc_v.shape[0] + n)]
    pltpu.make_async_copy(span, span, sem).wait()


def body(n_patch, n_sub, *args):
    nodes, edges, ced, wei, weo, wni, wno, fs, fr, hl, cs, cr = args
    fs, fr, cs, cr = (x.reshape(1, -1) for x in (fs, fr, cs, cr))
    operands = (nodes, edges, ced, wei, weo, wni, wno, fs, fr, hl, cs, cr)
    group = n_patch * n_sub
    n, d = nodes.shape
    e, c = edges.shape[0], ced.shape[0]
    halo = hl.shape[2]
    anywhere = pl.BlockSpec(memory_space=pl.ANY)
    inside = pl.BlockSpec(memory_space=pltpu.VMEM)
    dma = pltpu.SemaphoreType.DMA
    kept = [
        pltpu.VMEM((n, d), BF16),
        pltpu.VMEM((e, d), BF16),
        pltpu.VMEM((c, d), BF16),
        pltpu.VMEM((n, d), BF16),
        pltpu.VMEM((FIRST, d), F32),
        pltpu.VMEM((FIRST, d), F32),
        pltpu.VMEM(wni.shape, BF16),
        pltpu.VMEM(wno.shape, BF16),
    ]
    scratch = [pltpu.VMEM(x.shape, x.dtype) for x in (edges, ced, wei, weo, fs, fr, hl, cs, cr)] + [
        pltpu.VMEM((c, d), BF16),
        pltpu.VMEM((c, d), BF16),
        pltpu.VMEM((2,) + cs.shape, cs.dtype),
        pltpu.VMEM((group, CO_DEV, d), BF16),
        pltpu.VMEM((group * CO_DEV, d), F32),
        pltpu.VMEM((2, halo, d), BF16),
        pltpu.VMEM((2, halo, d), BF16),
        pltpu.VMEM((group * CO_DEV, d), F32),
        pltpu.VMEM((group, CO_DEV, d), BF16),
        pltpu.VMEM((group - n_sub, CO_DEV, d), BF16),
        pltpu.VMEM((e, d), F32),
        pltpu.VMEM((2 * c, d), F32),
        pltpu.VMEM(weo.shape, BF16),
        pltpu.VMEM(wno.shape, BF16),
        dma((3,)), dma, dma, dma, dma, dma, dma, dma, dma, pltpu.SemaphoreType.REGULAR,
    ]
    held = pl.pallas_call(
        functools.partial(kernel, n_patch, n_sub),
        out_shape=kept,
        in_specs=[anywhere] * len(operands),
        out_specs=[inside] * len(kept),
        scratch_shapes=scratch,
        compiler_params=pltpu.CompilerParams(
            collective_id=0, has_side_effects=True, vmem_limit_bytes=60 * 1024 * 1024),
        name="layer",
    )(*operands)
    return pl.pallas_call(
        finish,
        out_shape=[jax.ShapeDtypeStruct(x.shape, BF16) for x in (nodes, edges, ced)],
        in_specs=[inside] * len(kept),
        out_specs=[anywhere] * 3,
        scratch_shapes=[pltpu.VMEM((FIRST, d), BF16), dma],
        compiler_params=pltpu.CompilerParams(vmem_limit_bytes=8 * 1024 * 1024),
        name="finish",
    )(*held)


def solution(mesh):
    rows = P(("parts", "patch", "sub"), None)
    ids = P(("parts", "patch", "sub"))
    in_specs = (rows, rows, rows, P(), P(), P(), P(), ids, ids,
                P(("parts", "patch", "sub"), None, None), ids, ids)
    run = functools.partial(body, mesh.shape["patch"], mesh.shape["sub"])
    return jax.shard_map(run, mesh=mesh, in_specs=in_specs, out_specs=(rows, rows, rows),
                         check_vma=False)
```

```python
import functools

import jax
import jax.numpy as jnp
from jax import lax
from jax.experimental import pallas as pl
from jax.experimental.pallas import tpu as pltpu
from jax.sharding import PartitionSpec as P

CO_DEV = 4
FIRST = 8
F32 = jnp.float32
BF16 = jnp.bfloat16
MESH = pl.DeviceIdType.MESH


def dot(a, b, dims=((1,), (0,))):
    return lax.dot_general(a, b, (dims, ((), ())), preferred_element_type=F32)


def silu(v):
    half = 0.5 * v
    return (half + half * jnp.tanh(half)).astype(BF16)


def centre(w):
    n = w.shape[1]
    mean = dot(w, jnp.full((n, 128), 1.0, BF16)) * (1.0 / n)
    return jnp.concatenate(
        [(w[:, i:i + 128].astype(F32) - mean).astype(BF16) for i in range(0, n, 128)], axis=1)


def norm_rows(centred):
    return centred * lax.rsqrt(jnp.mean(centred * centred, axis=-1, keepdims=True) + 1e-05)


def column(row):
    n = row.shape[1]
    wide = jnp.broadcast_to(row.astype(F32), (8, n))
    return jnp.transpose(wide)[:, :1]


def hot(col, first, count):
    lanes = lax.broadcasted_iota(jnp.int32, (col.shape[0], count), 1) + first
    return (col == lanes.astype(F32)).astype(BF16)


def hot_t(row, count):
    rows = lax.broadcasted_iota(jnp.int32, (count, row.shape[1]), 0)
    return (rows == row).astype(BF16)


def each(count, step):
    if count <= 16:
        for i in range(count):
            step(i)
    else:
        def run(i, carry):
            step(i)
            return carry

        lax.fori_loop(0, count, run, 0)


def node_rows(rows, pre, w_out):
    return (rows.astype(F32) + norm_rows(dot(silu(pre), w_out))).astype(BF16)


def kernel(
    n_patch, n_sub,
    nodes_h, edges_h, ced_h, wei_h, weo_h, wni_h, wno_h, fs_h, fr_h, hl_h, cs_h, cr_h,
    n_rows, ne_v, nc_v, nodes_v, n_pre, top, wni_v, wno_v,
    edges_v, ced_v, wei_v, weo_v, fs_v, fr_v, hl_v, cs_v, cr_v,
    mate_v, mate_new, mate_ids,
    heads_r, heads_f, halo_s, halo_r, part_f, part_s, part_r,
    acc, ced_pre, weo_raw, wno_raw, in_sem, sent, ag_s, ag_r, halo_rs, rs_s, rs_r, ids_r, mate_r, near,
):
    group, shift = n_patch * n_sub, n_sub
    hub_p = n_patch - 1
    hubs = group - shift
    mp, ms = lax.axis_index("patch"), lax.axis_index("sub")
    me = mp * n_sub + ms
    hub, leaf, hosts = mp < hub_p, mp == hub_p, mp == hub_p - 1
    nodes_n, d = nodes_v.shape
    halo = halo_s.shape[1]
    co = heads_r.shape[1]
    count = ced_v.shape[0]

    def rows_of(i):
        start = i * 2 * co
        return pl.ds(start if isinstance(i, int) else pl.multiple_of(start, 2 * co), 2 * co)

    def turn(i, by, n):
        at = i + by
        return jnp.where(at >= n, at - n, at)

    def device(p, s):
        return {"device_id": {"patch": p, "sub": s}, "device_id_type": MESH}

    def device_of(i):
        if isinstance(i, int):
            return device(i // n_sub, i % n_sub)
        return device(lax.div(i, n_sub), lax.rem(i, n_sub))

    subs = [turn(ms, j, n_sub) for j in list(range(n_sub // 2, n_sub)) + list(range(1, n_sub // 2))]

    def patch(p, step):
        for s in subs + [ms]:
            step(p, s)

    def beside(step):
        for s in subs:
            step(mp, s)

    def await_rows(number, sem):
        span = heads_r.at[pl.ds(0, number)]
        pltpu.make_async_copy(span, span, sem).wait()

    barrier = pltpu.get_barrier_semaphore()

    def hail(p, s):
        pl.semaphore_signal(barrier, inc=1, **device(p, s))

    host, guest = device(jnp.maximum(mp - 1, 0), ms), device(jnp.minimum(mp + 1, hub_p), ms)
    visit = [
        pltpu.make_async_remote_copy(
            src_ref=src, dst_ref=dst, send_sem=out, recv_sem=sem, **host)
        for src, dst, out, sem in (
            (ced_h, mate_v, sent, mate_r),
            (cs_h, mate_ids.at[0], ids_r, ids_r), (cr_h, mate_ids.at[1], ids_r, ids_r))
    ]
    await_ids = pltpu.make_async_copy(mate_ids, mate_ids, ids_r).wait
    back = pltpu.make_async_remote_copy(
        src_ref=mate_new, dst_ref=mate_v, send_sem=sent, recv_sem=mate_r, **guest)

    @pl.when(hub)
    def _():
        patch(turn(mp, 1, hub_p), hail)
        pl.when(hosts)(lambda: hail(mp + 1, ms))
        each(hub_p - 2, lambda i: patch(turn(mp, i + 2, hub_p), hail))
        beside(hail)

    @pl.when(leaf)
    def _():
        pl.semaphore_wait(barrier, 1)
        for copy in visit:
            copy.start()

    groups = [
        [(nodes_h, nodes_v), (hl_h, hl_v)],
        [(fs_h, fs_v), (fr_h, fr_v), (cs_h, cs_v), (cr_h, cr_v), (wei_h, wei_v)],
        [(edges_h, edges_v), (ced_h, ced_v), (weo_h, weo_raw), (wni_h, wni_v), (wno_h, wno_raw)],
    ]
    loads = [[pltpu.make_async_copy(h, v, in_sem.at[i]) for h, v in pairs]
             for i, pairs in enumerate(groups)]
    for copies in loads:
        for copy in copies:
            copy.start()

    def loaded(i):
        for copy in loads[i]:
            copy.wait()

    loaded(0)
    nodes = nodes_v[...]
    head_row = heads_r.at[me]

    def send_head(p, s):
        pltpu.make_async_remote_copy(
            src_ref=head_row, dst_ref=head_row, send_sem=ag_s, recv_sem=ag_r,
            **device(p, s)).start()

    heads_r[me] = nodes[:co]

    @pl.when(hub)
    def _():
        pl.semaphore_wait(barrier, hubs - 1)
        pl.when(hosts)(lambda: hail(mp + 1, ms))
        each(hub_p - 1, lambda i: patch(turn(mp, hub_p - 1 - i, hub_p), send_head))
        beside(send_head)

    prev, after = turn(me, group - 1, group), turn(me, 1, group)

    def away(i):
        return jnp.where(i >= hubs, 1, 0)

    @pl.when(leaf)
    def _():
        pl.semaphore_wait(barrier, 1)
        each(hub_p, lambda i: patch(hub_p - 1 - i, send_head))
        pl.semaphore_signal(near, inc=1, **host)
        for i in (prev, after):
            pl.semaphore_signal(near, inc=1, **device_of(i - shift * away(i)))

    for side in range(2):
        pick = hot_t(hl_v[0, side:side + 1, :], nodes_n)
        halo_s[side] = dot(pick, nodes, ((0,), (0,))).astype(BF16)

    halos, soon = [], []
    for side, to in ((0, after), (1, prev)):
        soon.append(to < hubs)
        halos.append(pltpu.make_async_remote_copy(
            src_ref=halo_s.at[side], dst_ref=halo_r.at[side],
            send_sem=sent, recv_sem=halo_rs, **device_of(to)))
        pl.when(soon[-1])(halos[-1].start)

    loaded(1)
    fs, fr = fs_v[...], fr_v[...]
    fs_col = column(jnp.where(fs < halo, fs + (nodes_n + halo), fs - halo))
    fr_col = column(fr)
    own = jnp.concatenate(
        [dot(nodes, wei_v[d:2 * d]).astype(BF16), dot(nodes, wei_v[2 * d:]).astype(BF16)], axis=0)
    sel = jnp.concatenate([hot(fs_col, 0, nodes_n), hot(fr_col, 0, nodes_n)], axis=1)
    loaded(2)
    acc[...] = dot(edges_v[...], wei_v[:d]) + dot(sel, own)
    weo_v[...] = centre(weo_raw[...])
    wno_v[...] = centre(wno_raw[...])

    callers = away(prev) + away(after) + jnp.where(
        hosts, 1 + away(me + shift - 1) + away(turn(me + shift, 1, group)), 0)
    pl.when(hub & (callers > 0))(lambda: pl.semaphore_wait(near, callers))
    pl.when(hosts)(lambda: pl.semaphore_signal(near, inc=1, **guest))
    pl.when(leaf)(lambda: pl.semaphore_wait(near, 1))
    for early, copy in zip(soon, halos):
        pl.when(jnp.logical_not(early))(copy.start)

    def coarse(hosting):
        ced, cs, cr = ced_v[...], cs_v[...], cr_v[...]
        ced_pre[:count] = dot(ced, wei_v[:d])
        if hosting:
            await_ids()
            cs = jnp.concatenate([cs, mate_ids[0]], axis=1)
            cr = jnp.concatenate([cr, mate_ids[1]], axis=1)
        rows = cs.shape[1]
        picks = hot_t(cr, group * co)
        ends = jnp.concatenate(
            [hot(column(cs), 0, group * co), hot(column(cr), 0, group * co)], axis=0)
        if hosting:
            visit[0].wait_recv()
            ced_pre[count:] = dot(mate_v[...], wei_v[:d])
            ced = jnp.concatenate([ced, mate_v[...]], axis=0)

        await_rows(group - 1, ag_r)

        def flat(i):
            both = jnp.concatenate(
                [heads_r[2 * i].astype(F32), heads_r[2 * i + 1].astype(F32)], axis=0)
            heads_f[rows_of(i), :] = both

        each(group // 2, flat)
        heads = heads_f[...].astype(BF16)
        c_ends = dot(ends, heads).astype(BF16)
        c_in = jnp.concatenate([c_ends[:rows], c_ends[rows:]], axis=1)
        c_hid = silu(ced_pre[:rows] + dot(c_in, wei_v[d:]))
        c_new = (ced.astype(F32) + norm_rows(dot(c_hid, weo_v[...]))).astype(BF16)
        part_f[...] = dot(picks, c_new)

        if hosting:
            mate_new[...] = c_new[count:]

        def send_part(i):
            pltpu.make_async_remote_copy(
                src_ref=part_s.at[i], dst_ref=part_r.at[me],
                send_sem=rs_s, recv_sem=rs_r, **device_of(i)).start()

        def pack(i):
            both = part_f[rows_of(i), :].astype(BF16)
            part_s[2 * i] = both[:co]
            part_s[2 * i + 1] = both[co:]

        def send(i):
            for at in (2 * i, 2 * i + 1):
                pl.when(me != at)(lambda at=at: send_part(at))

        def pack_ahead(i):
            pack(i + 1)
            send(i)

        pack(0)
        each(group // 2 - 1, pack_ahead)
        send(group // 2 - 1)
        if hosting:
            back.start()
        part_r[me] = part_s[me]
        nc_v[...] = c_new[:count]

    pl.when(hub & jnp.logical_not(hosts))(lambda: coarse(False))
    pl.when(hosts)(lambda: coarse(True))

    pltpu.make_async_copy(halo_r, halo_r, halo_rs).wait()
    far = dot(jnp.concatenate([halo_r[1], halo_r[0]], axis=0), wei_v[d:2 * d]).astype(BF16)
    hid = silu(acc[...] + dot(hot(fs_col, nodes_n, 2 * halo), far))
    delta = norm_rows(dot(hid, weo_v[...]))
    e_new = (edges_v[...].astype(F32) + jnp.where(fr_col >= 0.0, delta, 0.0)).astype(BF16)
    ne_v[...] = e_new
    fine = dot(hot_t(fr, nodes_n), e_new)

    pre = dot(nodes, wni_v[:d])
    n_rows[...] = node_rows(nodes, pre + dot(fine.astype(BF16), wni_v[d:]), wno_v[...])
    first = top.shape[0]
    n_pre[...] = pre[:first]
    top[...] = fine[:first]

    def await_sent(rows):
        span = edges_v.at[pl.ds(0, rows)]
        pltpu.make_async_copy(span, span, sent).wait()

    pl.when(mp < hub_p - 1)(lambda: await_sent(2 * halo))
    pl.when(mp >= hub_p - 1)(lambda: await_sent(2 * halo + count))

    @pl.when(hub)
    def _():
        await_rows(hubs - 1, ag_s)
        await_rows(group - 1, rs_s)
        await_rows(hubs - 1, rs_r)

    @pl.when(leaf)
    def _():
        await_rows(hubs, ag_s)
        await_ids()
        back.wait_recv()
        nc_v[...] = mate_v[...]
        await_rows(hubs, rs_r)

    top[:co] += jnp.sum(part_r[...].astype(F32), axis=0)


def finish(n_rows, ne_v, nc_v, nodes_v, n_pre, top, wni_v, wno_v, nn_h, ne_h, nc_h, first_v, sem):
    first, d = top.shape
    n = n_rows.shape[0]
    for src, dst in (
            (ne_v, ne_h), (nc_v, nc_h),
            (n_rows.at[pl.ds(first, n - first)], nn_h.at[pl.ds(first, n - first)])):
        pltpu.make_async_copy(src, dst, sem).start()
    pre = n_pre[...] + dot(top[...].astype(BF16), wni_v[d:])
    first_v[...] = node_rows(nodes_v[:first], pre, wno_v[...])
    pltpu.make_async_copy(first_v, nn_h.at[pl.ds(0, first)], sem).start()
    span = wni_v.at[pl.ds(0, ne_v.shape[0] + nc_v.shape[0] + n)]
    pltpu.make_async_copy(span, span, sem).wait()


def body(n_patch, n_sub, *args):
    nodes, edges, ced, wei, weo, wni, wno, fs, fr, hl, cs, cr = args
    fs, fr, cs, cr = (x.reshape(1, -1) for x in (fs, fr, cs, cr))
    operands = (nodes, edges, ced, wei, weo, wni, wno, fs, fr, hl, cs, cr)
    group = n_patch * n_sub
    n, d = nodes.shape
    e, c = edges.shape[0], ced.shape[0]
    halo = hl.shape[2]
    anywhere = pl.BlockSpec(memory_space=pl.ANY)
    inside = pl.BlockSpec(memory_space=pltpu.VMEM)
    dma = pltpu.SemaphoreType.DMA
    kept = [
        pltpu.VMEM((n, d), BF16),
        pltpu.VMEM((e, d), BF16),
        pltpu.VMEM((c, d), BF16),
        pltpu.VMEM((n, d), BF16),
        pltpu.VMEM((FIRST, d), F32),
        pltpu.VMEM((FIRST, d), F32),
        pltpu.VMEM(wni.shape, BF16),
        pltpu.VMEM(wno.shape, BF16),
    ]
    scratch = [pltpu.VMEM(x.shape, x.dtype) for x in (edges, ced, wei, weo, fs, fr, hl, cs, cr)] + [
        pltpu.VMEM((c, d), BF16),
        pltpu.VMEM((c, d), BF16),
        pltpu.VMEM((2,) + cs.shape, cs.dtype),
        pltpu.VMEM((group, CO_DEV, d), BF16),
        pltpu.VMEM((group * CO_DEV, d), F32),
        pltpu.VMEM((2, halo, d), BF16),
        pltpu.VMEM((2, halo, d), BF16),
        pltpu.VMEM((group * CO_DEV, d), F32),
        pltpu.VMEM((group, CO_DEV, d), BF16),
        pltpu.VMEM((group - n_sub, CO_DEV, d), BF16),
        pltpu.VMEM((e, d), F32),
        pltpu.VMEM((2 * c, d), F32),
        pltpu.VMEM(weo.shape, BF16),
        pltpu.VMEM(wno.shape, BF16),
        dma((3,)), dma, dma, dma, dma, dma, dma, dma, dma, pltpu.SemaphoreType.REGULAR,
    ]
    held = pl.pallas_call(
        functools.partial(kernel, n_patch, n_sub),
        out_shape=kept,
        in_specs=[anywhere] * len(operands),
        out_specs=[inside] * len(kept),
        scratch_shapes=scratch,
        compiler_params=pltpu.CompilerParams(
            collective_id=0, has_side_effects=True, vmem_limit_bytes=60 * 1024 * 1024),
        name="layer",
    )(*operands)
    return pl.pallas_call(
        finish,
        out_shape=[jax.ShapeDtypeStruct(x.shape, BF16) for x in (nodes, edges, ced)],
        in_specs=[inside] * len(kept),
        out_specs=[anywhere] * 3,
        scratch_shapes=[pltpu.VMEM((FIRST, d), BF16), dma],
        compiler_params=pltpu.CompilerParams(vmem_limit_bytes=8 * 1024 * 1024),
        name="finish",
    )(*held)


def solution(mesh):
    rows = P(("parts", "patch", "sub"), None)
    ids = P(("parts", "patch", "sub"))
    in_specs = (rows, rows, rows, P(), P(), P(), P(), ids, ids,
                P(("parts", "patch", "sub"), None, None), ids, ids)
    run = functools.partial(body, mesh.shape["patch"], mesh.shape["sub"])
    return jax.shard_map(run, mesh=mesh, in_specs=in_specs, out_specs=(rows, rows, rows),
                         check_vma=False)
```
